128 devices in a mesh: gx: 4 (over x), gy: 4 (over y_lo, core), gz: 8 (over z, y_hi).
Axes of the slice: x: 4, y: 4 (y_hi: 2, y_lo: 2; y = y_hi * 2 + y_lo), z: 4, core: 2. Of those that a mesh axis runs over, the one named last changes fastest.
Arguments:
- layer_input: bfloat16 [4096, 4096], P('gz', ('gx', 'gy')), may hold values from -6 to 6
- modality: int32 [4096], P('gz'), may hold values 0 or 1
- image_spans: int32 [2, 8], replicated, may hold values from 0 to 4096, as said below
- norm_gain: float32 [2, 4096], P(None, ('gx', 'gy')), may hold values from 0.1 to 1.9
- w_qkv: bfloat16 [3, 4096, 2048], P(None, 'gz', ('gx', 'gy')), as said below
- w_out: bfloat16 [2048, 4096], P(('gx', 'gy'), 'gz'), may hold values from -0.125 to 0.125
- grad_out: bfloat16 [4096, 4096], P('gz', ('gx', 'gy')), may hold values from -6 to 6
Outputs:
- attn_out: bfloat16 [4096, 4096], P('gz', ('gx', 'gy'))
- grad_in: bfloat16 [4096, 4096], P('gz', ('gx', 'gy'))
- grad_qkv: float32 [3, 4096, 2048], P(None, 'gz', ('gx', 'gy'))
- grad_wout: float32 [2048, 4096], P(('gx', 'gy'), 'gz')
- grad_gain: float32 [2, 4096], P(None, ('gx', 'gy'))
The draws below stay inside these ranges and needn't reach their ends.
Inputs may be any that keep to these rules, and one draw needn't show every extreme that they name: `image_spans`: row 0 holds the first position of each of 8 image spans, in increasing order, and row 1 one past its last; spans are disjoint and none is empty. `w_qkv`: entries are at most 20 * 4096 ** -0.5 in magnitude.
All inputs are finite; a program needn't handle non-finite values. No bound on the sum of `modality` on one device may be relied on, other than what follows from the above.
Results may differ from the reference program's by a relative error of at most 0.035.
The reference program's roundings to bfloat16 on the way (of `normed`, `queries`, `attended`, `d_attended`, `d_scores`, `d_queries` and `d_keys`) count: a program that leaves them out, or rounds other values in their place, can miss the bound.
Values may be sent and summed in bfloat16 or wider, within the bound.
No kernel may reach another device: no remote copies, remote signals or barrier semaphores. Data moves between devices by JAX's collectives and lax.ppermute only.
A program may use at most 128 MiB of HBM per device.

```python
import math
import jax
import jax.numpy as jnp
from jax import lax

D = 4096
HEAD_DIM = 128
TOK_DEV = 512
SPANS = 8
HEADS = 16
TOKENS = 4096
N_GX = 4
N_GY = 4
N_GZ = 8


def draw_image_spans(key, part):
    stride = TOKENS // SPANS
    key_one, key_two = jax.random.split(jax.random.fold_in(key, 11))
    labels = jnp.arange(SPANS, dtype=jnp.int32)
    offset = jax.random.randint(key_one, (SPANS,), 0, max(stride // 4, 1))
    length = jax.random.randint(key_two, (SPANS,), max(stride // 4, 1), stride // 2 + 1)
    starts = labels * stride + stride // 2 + offset
    finish = jnp.minimum(starts + length, TOKENS)
    return jnp.stack([starts, finish]).astype(jnp.int32)


def draw_w_qkv(key, part):
    key_one = jax.random.fold_in(jax.random.fold_in(key, 23), 0)
    weights = jax.random.truncated_normal(key_one, -4.0, 4.0, (3, D, HEADS * HEAD_DIM), jnp.float32) * D ** (-0.5)
    return weights.astype(jnp.bfloat16)


def with_ends(entries, stream_key, least, top_value):
    longest = entries.shape.index(max(entries.shape))
    spots = []
    for shift in (0, 1):
        where = [jax.random.randint(jax.random.fold_in(stream_key, axis), (), 0, length) for axis, length in enumerate(entries.shape)]
        where[longest] = (where[longest] + shift) % entries.shape[longest]
        spots.append(tuple(where))
    return entries.at[spots[0]].set(least).at[spots[1]].set(top_value)


def level_of(rng, dims, cuts, smallest, high):
    loudness = 1.0
    for position, blocks in cuts:
        steps = jax.random.uniform(jax.random.fold_in(jax.random.fold_in(rng, 6), position), (blocks,), jnp.float32, smallest / len(cuts), high / len(cuts))
        loudness = loudness * jnp.repeat(jnp.exp(steps), dims[position] // blocks).reshape((-1,) + (1,) * (len(dims) - 1 - position))
    return loudness


def scatter_about(own_key, shape, deviation, bound, cuts=(), kind=jnp.bfloat16):
    drawn = jax.random.normal(own_key, shape, jnp.float32) * deviation
    if len(cuts) > 0:
        drawn = level_of(own_key, shape, cuts, -0.22, 0.18) * drawn
    return jnp.clip(drawn, min=-bound, max=bound).astype(kind)


def setup_inputs(seed: int = 0) -> dict:
    splits = jax.random.split(jax.random.key(seed), 8)
    return {
        "layer_input": scatter_about(splits[0], (TOKENS, D), 1.0, 6.0, ((0, 8), (1, 16))),
        "modality": with_ends((jax.random.randint(splits[1], (TOKENS,), 0, 2) < 1).astype(jnp.int32), jax.random.fold_in(splits[1], 1), 0, 1),
        "image_spans": draw_image_spans(jax.random.fold_in(splits[7], 71), 0),
        "norm_gain": jnp.clip(1.0 + 0.18 * jax.random.normal(splits[3], (2, D), jnp.float32), 0.1, 1.9),
        "w_qkv": draw_w_qkv(jax.random.fold_in(splits[7], 71), 0),
        "w_out": scatter_about(splits[5], (HEADS * HEAD_DIM, D), (HEADS * HEAD_DIM) ** -0.5, 0.125, ((0, 16), (1, 8))),
        "grad_out": scatter_about(splits[6], (TOKENS, D), 1.0, 6.0, ((0, 8), (1, 16))),
    }


epsilon = 1e-05
masked_low = -1e+30

def span_index(positions, image_spans):
    inside = (positions[:, None] >= image_spans[0][None, :]) & (positions[:, None] < image_spans[1][None, :])
    labels = jnp.arange(1, image_spans.shape[1] + 1, dtype=jnp.int32)
    return (lax.optimization_barrier(jnp.sum(jnp.where(inside, labels[None, :], 0), axis=1)) - 1).astype(jnp.int32)

def visible(query_pos, query_span, key_pos, key_span):
    causal = key_pos[None, :] <= query_pos[:, None]
    same_image = (query_span[:, None] == key_span[None, :]) & (query_span[:, None] >= 0)
    return causal | same_image

def rounded(value):
    return lax.optimization_barrier(value.astype(jnp.bfloat16)).astype(jnp.float32)

def reference(layer_input, modality, image_spans, norm_gain, w_qkv, w_out, grad_out):
    full_width = layer_input.shape[1]
    head_count = N_GX * N_GY
    inputs_f = layer_input.astype(jnp.float32)
    inv_rms = lax.rsqrt(lax.optimization_barrier(jnp.mean(inputs_f * inputs_f, axis=1)) + epsilon)
    row_gain = jnp.where(modality[:, None] == 1, norm_gain[1][None, :], norm_gain[0][None, :])
    scaled = inputs_f * inv_rms[:, None]
    normed = (scaled * row_gain).astype(jnp.bfloat16)
    projected = [jnp.dot(normed, w_qkv[matrix_idx], preferred_element_type=jnp.float32).astype(jnp.bfloat16) for matrix_idx in range(3)]
    positions = jnp.arange(TOKENS, dtype=jnp.int32)
    span_ids = span_index(positions, image_spans)
    allowed = visible(positions, span_ids, positions, span_ids)
    d_attended = jnp.dot(grad_out, w_out.T, preferred_element_type=jnp.float32).astype(jnp.bfloat16)
    score_scale = 1.0 / math.sqrt(HEAD_DIM)

    def split_heads(matrix):
        return matrix.reshape(TOKENS, head_count, HEAD_DIM).transpose(1, 0, 2)

    def merge_heads(stacked):
        return stacked.transpose(1, 0, 2).reshape(TOKENS, head_count * HEAD_DIM)

    def one_head(operands):
        queries, keys, values, d_head = operands
        scores = jnp.dot(queries, keys.T, preferred_element_type=jnp.float32) * score_scale
        maxima = lax.optimization_barrier(jnp.max(jnp.where(allowed, scores, masked_low), axis=1))
        summed = lax.optimization_barrier(jnp.sum(jnp.where(allowed, jnp.exp(scores - maxima[:, None]), 0.0), axis=1))
        lse = maxima + jnp.log(summed)
        attn_p = jnp.where(allowed, jnp.exp(scores - lse[:, None]), 0.0)
        attn_pb = attn_p.astype(jnp.bfloat16)
        attended = jnp.dot(attn_pb, values, preferred_element_type=jnp.float32).astype(jnp.bfloat16)
        row_dots = lax.optimization_barrier(jnp.sum(d_head.astype(jnp.float32) * attended.astype(jnp.float32), axis=1))
        d_probs = jnp.dot(d_head, values.T, preferred_element_type=jnp.float32)
        d_scores = (attn_p * (d_probs - row_dots[:, None]) * score_scale).astype(jnp.bfloat16)
        d_queries = jnp.dot(d_scores, keys, preferred_element_type=jnp.float32).astype(jnp.bfloat16)
        score_blocks = d_scores.reshape(N_GZ, TOK_DEV, TOKENS).astype(jnp.float32)
        prob_blocks = attn_pb.reshape(N_GZ, TOK_DEV, TOKENS).astype(jnp.float32)
        query_blocks = queries.reshape(N_GZ, TOK_DEV, HEAD_DIM).astype(jnp.float32)
        upstream_blocks = d_head.reshape(N_GZ, TOK_DEV, HEAD_DIM).astype(jnp.float32)
        key_parts = jnp.einsum('gik,gid->gkd', score_blocks, query_blocks)
        value_parts = jnp.einsum('gik,gid->gkd', prob_blocks, upstream_blocks)
        d_keys = lax.optimization_barrier(jnp.sum(rounded(key_parts), axis=0)).astype(jnp.bfloat16)
        d_values = lax.optimization_barrier(jnp.sum(rounded(value_parts), axis=0)).astype(jnp.bfloat16)
        return (attended, d_queries, d_keys, d_values)
    results = lax.map(one_head, (split_heads(projected[0]), split_heads(projected[1]), split_heads(projected[2]), split_heads(d_attended)))
    attended = merge_heads(results[0])
    grads = [merge_heads(results[1]), merge_heads(results[2]), merge_heads(results[3])]
    branch = jnp.zeros((TOKENS, full_width), jnp.float32)
    grad_normed = jnp.zeros((TOKENS, full_width), jnp.float32)
    for head in range(head_count):
        columns = slice(head * HEAD_DIM, (head + 1) * HEAD_DIM)
        branch = branch + rounded(jnp.dot(attended[:, columns], w_out[columns], preferred_element_type=jnp.float32))
        partial_value = jnp.zeros((TOKENS, full_width), jnp.float32)
        for matrix_idx in range(3):
            partial_value = partial_value + jnp.dot(grads[matrix_idx][:, columns], w_qkv[matrix_idx][:, columns].T, preferred_element_type=jnp.float32)
        grad_normed = grad_normed + rounded(partial_value)
    attn_out = branch.astype(jnp.bfloat16)
    grad_wout = jnp.zeros((head_count * HEAD_DIM, full_width), jnp.float32)
    qkv_parts = [jnp.zeros((full_width, head_count * HEAD_DIM), jnp.float32) for matrix_idx in range(3)]
    for group in range(N_GZ):
        tok_rows = slice(group * TOK_DEV, (group + 1) * TOK_DEV)
        grad_wout = grad_wout + rounded(jnp.dot(attended[tok_rows].T, grad_out[tok_rows], preferred_element_type=jnp.float32))
        for matrix_idx in range(3):
            qkv_parts[matrix_idx] = qkv_parts[matrix_idx] + rounded(jnp.dot(normed[tok_rows].T, grads[matrix_idx][tok_rows], preferred_element_type=jnp.float32))
    grad_qkv = jnp.stack(qkv_parts)
    upstream = grad_normed * row_gain
    norm_dots = lax.optimization_barrier(jnp.mean(upstream * scaled, axis=1))
    grad_in = (inv_rms[:, None] * (upstream - scaled * norm_dots[:, None])).astype(jnp.bfloat16)
    onehot = (modality[:, None] == jnp.arange(2, dtype=jnp.int32)[None, :]).astype(jnp.float32)
    grad_gain = jnp.dot(onehot.T, grad_normed * scaled, precision=lax.Precision.HIGHEST)
    return (attn_out, grad_in, grad_qkv, grad_wout, grad_gain)
```

```python
import math

import jax
import jax.numpy as jnp
from jax import lax
from jax.experimental import pallas as pl
from jax.experimental.pallas import tpu as pltpu
from jax.sharding import Mesh
from jax.sharding import PartitionSpec as P


epsilon = 1e-05
masked_low = -1e30
GROUP = ("x", "h", "c")
TOKENS_AXES = ("z", "u")
F32 = jnp.float32
BF16 = jnp.bfloat16
TURNS = (0, 1, 3, 2)
NT = (((1,), (1,)), ((), ()))
TN = (((0,), (0,)), ((), ()))
SMEM = pl.BlockSpec(memory_space=pltpu.SMEM)
PARAMS = pltpu.CompilerParams(vmem_limit_bytes=60 * 1024 * 1024)


def swap(a, axis):
    return lax.ppermute(a, axis, [(0, 1), (1, 0)])


def turn(a, d):
    return lax.ppermute(a, "x", [(i, (i + d) % 4) for i in range(4)])


def spread(block):
    pair = jnp.stack([block, swap(block, "h")])
    own = [pair] + [turn(pair, d) for d in TURNS[1:]]
    return own + [swap(a, "c") for a in own]


def to_all(x, axis):
    length = lax.axis_size(axis)
    return lax.all_to_all(jnp.broadcast_to(x[None], (length, *x.shape)), axis, 0, 0, tiled=True)


def three_parts(g):
    high = lax.reduce_precision(g, 8, 7)
    rest = g - high
    mid = lax.reduce_precision(rest, 8, 7)
    return high, mid, rest - mid


def dot(a, b, dims=(((1,), (0,)), ((), ()))):
    return lax.dot_general(a, b, dims, preferred_element_type=F32)


def project_kernel(idx, *refs):
    xs, gains = refs[:8], refs[8:16]
    mod, w, normed, q, kv, inv_out, acc = refs[16:]
    rows = q.shape[0]
    squares = jnp.zeros((rows, 256), F32)
    for a in xs:
        for s in range(2):
            xb = a[s].astype(F32)
            squares = squares + xb * xb
    inv = lax.rsqrt(jnp.sum(squares, axis=1, keepdims=True) / 4096 + epsilon)
    inv_out[...] = inv
    second = mod[...] == 1
    acc[...] = jnp.zeros_like(acc)
    for n in range(16):
        a, s = n // 2, n % 2
        g = gains[a][s].astype(F32)
        g0 = (g[0:1] + g[2:3]) + g[4:5]
        g1 = (g[1:2] + g[3:4]) + g[5:6]
        nb = ((xs[a][s].astype(F32) * inv) * jnp.where(second, g1, g0)).astype(BF16)
        j = idx[n]
        normed[j] = nb
        acc[...] += dot(nb, w[j, 0:384, :], NT)
    out = acc[...].astype(BF16)
    q[...] = out[:, 0:128]
    kv[...] = out[:, 128:384]


def project(idx, xs, modality, wcat):
    tile = 128
    whole = lambda *shape: pl.BlockSpec(shape, lambda i: (0,) * len(shape))
    rows = lambda cols: pl.BlockSpec((tile, cols), lambda i: (i, 0))
    return pl.pallas_call(
        project_kernel,
        name="project",
        grid=(512 // tile,),
        in_specs=[SMEM]
        + [pl.BlockSpec((2, tile, 256), lambda i: (0, i, 0))] * 8
        + [pl.BlockSpec((2, 16, 256), lambda i: (0, 32, 0))] * 8
        + [rows(1), whole(16, 512, 256)],
        out_specs=[
            pl.BlockSpec((16, tile, 256), lambda i: (0, i, 0)),
            rows(128),
            rows(256),
            rows(1),
        ],
        out_shape=[
            jax.ShapeDtypeStruct((16, 512, 256), BF16),
            jax.ShapeDtypeStruct((512, 128), BF16),
            jax.ShapeDtypeStruct((512, 256), BF16),
            jax.ShapeDtypeStruct((512, 1), F32),
        ],
        scratch_shapes=[pltpu.VMEM((tile, 384), F32)],
        compiler_params=PARAMS,
    )(idx, *xs, *xs, modality[:, None], wcat)


def upstream_kernel(idx, *refs):
    gs, w, out = refs[:8], refs[8], refs[9]
    acc = jnp.zeros(out.shape, F32)
    for n in range(16):
        acc = acc + dot(gs[n // 2][n % 2], w[idx[n]], NT)
    out[...] = acc.astype(BF16)


def upstream(idx, gs, wcat):
    tile = 128
    return pl.pallas_call(
        upstream_kernel,
        name="upstream",
        grid=(512 // tile,),
        in_specs=[SMEM]
        + [pl.BlockSpec((2, tile, 256), lambda i: (0, i, 0))] * 8
        + [pl.BlockSpec((16, 128, 256), lambda i: (0, 3, 0))],
        out_specs=pl.BlockSpec((tile, 128), lambda i: (i, 0)),
        out_shape=jax.ShapeDtypeStruct((512, 128), BF16),
        compiler_params=PARAMS,
    )(idx, *gs, wcat)


def attention_kernel(limit, q, kv, da, att, att_t, dq, dkv, s_all, p_all):
    block = 512
    count = kv.shape[0] // block
    scale = 1.0 / math.sqrt(q.shape[1])
    to_base2 = scale * math.log2(math.e)
    cols = q.shape[0]
    edge = limit[...]

    def scores(b, top):
        at = pl.ds(b * block, block)
        s = dot(kv[at, 0:128], q[...], NT) * to_base2
        pos = lax.broadcasted_iota(jnp.int32, s.shape, 0) + b * block
        s = jnp.where(pos < edge, s, masked_low)
        s_all[at, :] = s
        return jnp.maximum(top, jnp.max(s, axis=0, keepdims=True))

    top = lax.fori_loop(0, count, scores, jnp.full((1, cols), masked_low, F32))

    def sums(b, total):
        at = pl.ds(b * block, block)
        e = jnp.exp2(s_all[at, :] - top)
        s_all[at, :] = e
        return total + jnp.sum(e, axis=0, keepdims=True)

    total = lax.fori_loop(0, count, sums, jnp.zeros((1, cols), F32))
    inv = 1.0 / total

    def attend(b, acc):
        at = pl.ds(b * block, block)
        p = (s_all[at, :] * inv).astype(BF16)
        p_all[at, :] = p
        return acc + dot(kv[at, 128:256], p, TN)

    out_t = lax.fori_loop(0, count, attend, jnp.zeros((128, cols), F32)).astype(BF16)
    att_t[...] = out_t
    att[...] = out_t.T
    da_t = da[...].T
    row_dots = jnp.sum(out_t.astype(F32) * da_t.astype(F32), axis=0, keepdims=True)

    def back(b, acc):
        at = pl.ds(b * block, block)
        d_probs = dot(kv[at, 128:256], da[...], NT)
        ds = ((s_all[at, :] * inv) * (d_probs - row_dots) * scale).astype(BF16)
        dkv[at, 0:128] = dot(ds, q[...]).astype(BF16)
        dkv[at, 128:256] = dot(p_all[at, :], da[...]).astype(BF16)
        return acc + dot(kv[at, 0:128], ds, TN)

    dq_t = lax.fori_loop(0, count, back, jnp.zeros((128, cols), F32))
    dq[...] = dq_t.astype(BF16).T


def attention(limit, q, kv, da):
    shape = jax.ShapeDtypeStruct
    return pl.pallas_call(
        attention_kernel,
        name="attention",
        out_shape=[
            shape((512, 128), BF16),
            shape((128, 512), BF16),
            shape((512, 128), BF16),
            shape((4096, 256), BF16),
        ],
        scratch_shapes=[pltpu.VMEM((4096, 512), F32), pltpu.VMEM((4096, 512), BF16)],
        compiler_params=PARAMS,
    )(limit, q, kv, da)


def put_parts(ref, at, dots):
    parts = [dots[:, 0:256], dots[:, 256:512]]
    rows = []
    for p in parts:
        high = p.astype(BF16).astype(F32)
        mid = (p - high).astype(BF16).astype(F32)
        rows.append((high, mid, p - high - mid))
    kind = lax.broadcasted_iota(jnp.int32, (16, 256), 0)
    both = jnp.zeros((16, 256), F32)
    for r in range(6):
        both = jnp.where(kind == r, rows[r % 2][r // 2], both)
    ref[at, 512:528, :] = both.astype(BF16)


def get_parts(block):
    t = block.astype(F32)
    return (t[0:2] + t[2:4]) + t[4:6]


def input_grad_kernel(sent_idx, kept_idx, dkv, dq, q, kv, w, sent, kept, g_t):
    total = dkv[0].astype(F32)
    for k in range(1, 8):
        total = total + dkv[k].astype(F32)
    gkv = total.astype(BF16)
    g = jnp.concatenate([dq[...], gkv], axis=1)
    g_t[...] = g.T
    gf = g.astype(F32)
    prod = gf[:, 0:128] * q[...].astype(F32)
    prod = prod + gf[:, 128:256] * kv[:, 0:128].astype(F32)
    prod = prod + gf[:, 256:384] * kv[:, 128:256].astype(F32)
    dots = lax.dot_general(
        jnp.ones((8, 128), F32), prod, NT, precision=lax.Precision.HIGHEST, preferred_element_type=F32
    )[0:1]

    for ref, idx in ((sent, sent_idx), (kept, kept_idx)):

        def one(n, carry, ref=ref, idx=idx):
            ref[n, 0:512, :] = dot(g, w[idx[n], 0:384, :]).astype(BF16)
            put_parts(ref, n, dots)
            return carry

        lax.fori_loop(0, 8, one, 0)


def input_grad(sent_idx, kept_idx, dkv, dq, q, kv, wcat):
    shape = jax.ShapeDtypeStruct
    vmem = pl.BlockSpec(memory_space=pltpu.VMEM)
    return pl.pallas_call(
        input_grad_kernel,
        name="input_grad",
        in_specs=[SMEM, SMEM] + [vmem] * 5,
        out_shape=[
            shape((8, 528, 256), BF16),
            shape((8, 528, 256), BF16),
            shape((384, 512), BF16),
        ],
        compiler_params=PARAMS,
    )(sent_idx, kept_idx, dkv, dq, q, kv, wcat)


def weight_grad_kernel(idx, *refs):
    gs, normed, g_t, att_t, out = refs[:8], refs[8], refs[9], refs[10], refs[11]

    def one(j, carry):
        out[j, 0:384, :] = dot(g_t[...], normed[j]).astype(BF16)
        return carry

    lax.fori_loop(0, 16, one, 0)
    for n in range(16):
        out[idx[n], 384:512, :] = dot(att_t[...], gs[n // 2][n % 2]).astype(BF16)


def weight_grad(idx, gs, normed, g_t, att_t):
    vmem = pl.BlockSpec(memory_space=pltpu.VMEM)
    return pl.pallas_call(
        weight_grad_kernel,
        name="weight_grad",
        in_specs=[SMEM] + [vmem] * 11,
        out_shape=jax.ShapeDtypeStruct((16, 512, 256), BF16),
        compiler_params=PARAMS,
    )(idx, *gs, normed, g_t, att_t)


def add_up_kernel(*refs):
    terms, out = refs[:-1], refs[-1]
    total = terms[0][0, 0:512].astype(F32)
    dots = get_parts(terms[0][0, 512:528])
    for t in terms[1:]:
        total = total + t[0, 0:512].astype(F32)
        dots = dots + get_parts(t[0, 512:528])
    out[0, 0:512] = total.astype(BF16)
    put_parts(out, 0, jnp.concatenate([dots[0:1], dots[1:2]], axis=1))


def add_up(terms):
    count = terms[0].shape[0]
    spec = pl.BlockSpec((1, 528, 256), lambda i: (i, 0, 0))
    return pl.pallas_call(
        add_up_kernel,
        name="add_up",
        grid=(count,),
        in_specs=[spec] * len(terms),
        out_specs=spec,
        out_shape=jax.ShapeDtypeStruct((count, 528, 256), BF16),
        compiler_params=PARAMS,
    )(*terms)


def finish_kernel(one, two, x, inv, mod, gain, grad_in, local_gain):
    gn = one[0:512].astype(F32) + two[0:512].astype(F32)
    dots = get_parts(one[512:528]) + get_parts(two[512:528])
    columns = [jnp.broadcast_to(dots[r : r + 1], (128, 256)).T[:, 0:1] for r in range(2)]
    mean = jnp.concatenate(columns, axis=0) / 4096
    second = mod[...] == 1
    scaled = x[...].astype(F32) * inv[...]
    up = gn * jnp.where(second, gain[1:2], gain[0:1])
    grad_in[...] = (inv[...] * (up - scaled * mean)).astype(BF16)
    terms = gn * scaled
    local_gain[0:1] = jnp.sum(jnp.where(second, 0.0, terms), axis=0, keepdims=True)
    local_gain[1:2] = jnp.sum(jnp.where(second, terms, 0.0), axis=0, keepdims=True)


def finish(one, two, x, inv, modality, gain):
    return pl.pallas_call(
        finish_kernel,
        name="finish",
        out_shape=[
            jax.ShapeDtypeStruct((512, 256), BF16),
            jax.ShapeDtypeStruct((2, 256), F32),
        ],
        compiler_params=PARAMS,
    )(one, two, x, inv, modality[:, None], gain)


def output_kernel(idx, *refs):
    atts, rows, out = refs[:8], refs[8], refs[9]
    total = jnp.zeros(out.shape, F32)
    for n in range(16):
        total = total + dot(atts[n // 2][n % 2], rows[idx[n]]).astype(BF16).astype(F32)
    out[...] = total.astype(BF16)


def output(idx, atts, rows):
    tile = 128
    return pl.pallas_call(
        output_kernel,
        name="output",
        grid=(512 // tile,),
        in_specs=[SMEM]
        + [pl.BlockSpec((2, tile, 128), lambda i: (0, i, 0))] * 8
        + [pl.BlockSpec((16, 128, 256), lambda i: (0, 0, 0))],
        out_specs=pl.BlockSpec((tile, 256), lambda i: (i, 0)),
        out_shape=jax.ShapeDtypeStruct((512, 256), BF16),
        compiler_params=PARAMS,
    )(idx, *atts, rows)


def sum_weights_kernel(parts, qkv, wout):
    total = parts[0, 0].astype(F32)
    for k in range(1, 8):
        total = total + parts[k, 0].astype(F32)
    for m in range(3):
        qkv[m] = total[m * 128 : (m + 1) * 128].T
    wout[...] = total[384:512]


def sum_weights(parts):
    return pl.pallas_call(
        sum_weights_kernel,
        name="sum_weights",
        grid=(2,),
        in_specs=[pl.BlockSpec((8, 1, 512, 256), lambda s: (0, s, 0, 0))],
        out_specs=[
            pl.BlockSpec((3, 256, 128), lambda s: (0, s, 0)),
            pl.BlockSpec((128, 256), lambda s: (0, s)),
        ],
        out_shape=[
            jax.ShapeDtypeStruct((3, 512, 128), F32),
            jax.ShapeDtypeStruct((128, 512), F32),
        ],
        compiler_params=PARAMS,
    )(parts)


def per_device(layer_input, modality, image_spans, norm_gain, w_qkv, w_out, grad_out):
    x, h, c = (lax.axis_index(a) for a in GROUP)
    blocks = [((x - d) % 4, h ^ s, c ^ k) for k in range(2) for d in TURNS for s in range(2)]
    idx = jnp.stack([a * 4 + b * 2 + e for a, b, e in blocks]).astype(jnp.int32)
    places = [((x + d) % 4, h ^ s) for d in range(4) for s in range(2)]
    kept_idx = jnp.stack([a * 4 + b * 2 + c for a, b in places]).astype(jnp.int32)
    sent_idx = jnp.stack([a * 4 + b * 2 + (1 - c) for a, b in places]).astype(jnp.int32)

    w_t = w_qkv.transpose(0, 2, 1).reshape(384, 512)
    both = jnp.concatenate([w_t, w_out], axis=0)
    halves = jnp.stack([both[:, 0:256], both[:, 256:512]])
    wcat = to_all(halves, TOKENS_AXES).reshape(16, 512, 256)

    gain_rows = jnp.concatenate(three_parts(norm_gain), axis=0).astype(BF16)
    gain_rows = jnp.concatenate([gain_rows, jnp.zeros((10, 256), BF16)], axis=0)
    xs = spread(jnp.concatenate([layer_input, gain_rows], axis=0))
    normed, q, kv, inv = project(idx, xs, modality, wcat)

    all_kv = to_all(kv, TOKENS_AXES).reshape(4096, 256)
    gs = spread(grad_out)
    da = upstream(idx, gs, wcat)

    pos = lax.axis_index(TOKENS_AXES) * 512 + jnp.arange(512, dtype=jnp.int32)
    inside = (pos[:, None] >= image_spans[0][None]) & (pos[:, None] < image_spans[1][None])
    ends = jnp.max(jnp.where(inside, image_spans[1][None], 0), axis=1)
    limit = jnp.maximum(pos + 1, ends)[None, :]

    att, att_t, dq, dkv = attention(limit, q, all_kv, da)

    out_rows = lax.all_to_all(wcat[:, 384:512, :], GROUP, 0, 0, tiled=True)
    attn_out = output(idx, spread(att), out_rows)

    dkv_parts = lax.all_to_all(dkv.reshape(8, 512, 256), TOKENS_AXES, 0, 0, tiled=True)
    sent, kept, g_t = input_grad(sent_idx, kept_idx, dkv_parts, dq, q, kv, wcat)
    chip = add_up([kept, swap(sent, "c")])
    pairs = [chip[0:2]] + [turn(chip[2 * d : 2 * d + 2], d) for d in (1, 2, 3)]
    line = add_up(pairs)
    last = swap(line[1], "h")
    grad_in, local_gain = finish(line[0], last, layer_input, inv, modality, norm_gain)

    w_parts = weight_grad(idx, gs, normed, g_t, att_t).reshape(8, 2, 512, 256)
    w_parts = lax.all_to_all(w_parts, TOKENS_AXES, 0, 0, tiled=True)
    grad_qkv, grad_wout = sum_weights(w_parts)
    grad_gain = jnp.sum(to_all(local_gain, TOKENS_AXES), axis=0)
    return (attn_out, grad_in, grad_qkv, grad_wout, grad_gain)


def solution(mesh):
    fine = Mesh(mesh.devices.reshape(4, 2, 2, 4, 2), ("x", "h", "c", "z", "u"))
    tok, feat = TOKENS_AXES, GROUP
    in_specs = (P(tok, feat), P(tok), P(), P(None, feat), P(None, tok, feat), P(feat, tok), P(tok, feat))
    out_specs = (P(tok, feat), P(tok, feat), P(None, tok, feat), P(feat, tok), P(None, feat))
    return jax.shard_map(per_device, mesh=fine, in_specs=in_specs, out_specs=out_specs, check_vma=False)
```

```python
import math

import jax
import jax.numpy as jnp
from jax import lax
from jax.experimental import pallas as pl
from jax.experimental.pallas import tpu as pltpu
from jax.sharding import Mesh
from jax.sharding import PartitionSpec as P


epsilon = 1e-05
masked_low = -1e30
GROUP = ("x", "h", "c")
TOKENS_AXES = ("z", "u")
F32 = jnp.float32
BF16 = jnp.bfloat16
TURNS = (0, 1, 3, 2)
NT = (((1,), (1,)), ((), ()))
TN = (((0,), (0,)), ((), ()))
SMEM = pl.BlockSpec(memory_space=pltpu.SMEM)
PARAMS = pltpu.CompilerParams(vmem_limit_bytes=60 * 1024 * 1024)


def swap(a, axis):
    return lax.ppermute(a, axis, [(0, 1), (1, 0)])


def turn(a, d):
    return lax.ppermute(a, "x", [(i, (i + d) % 4) for i in range(4)])


def spread(block):
    pair = jnp.stack([block, swap(block, "h")])
    own = [pair] + [turn(pair, d) for d in TURNS[1:]]
    return own + [swap(a, "c") for a in own]


def exchange(blocks, axis):
    return lax.all_to_all(blocks, axis, 0, 0, tiled=True)


def copies(x, count):
    return jnp.broadcast_to(x[None], (count, *x.shape))


def three_parts(g):
    high = lax.reduce_precision(g, 8, 7)
    rest = g - high
    mid = lax.reduce_precision(rest, 8, 7)
    return high, mid, rest - mid


def dot(a, b, dims=(((1,), (0,)), ((), ()))):
    return lax.dot_general(a, b, dims, preferred_element_type=F32)


def shape(dims, kind=BF16):
    return jax.ShapeDtypeStruct(dims, kind)


def fixed(*dims):
    return pl.BlockSpec(dims, lambda *i: (0,) * len(dims))


def pack_kernel(w, out):
    for m in range(3):
        block = w[m].T
        for k in range(8):
            out[k, 0, m * 128 : (m + 1) * 128, :] = block


def pack_weights(w):
    return pl.pallas_call(
        pack_kernel,
        name="pack_weights",
        grid=(2,),
        in_specs=[pl.BlockSpec((3, 256, 128), lambda s: (0, s, 0))],
        out_specs=pl.BlockSpec((8, 1, 384, 256), lambda s: (0, s, 0, 0)),
        out_shape=shape((8, 2, 384, 256)),
        compiler_params=PARAMS,
    )(w)


def normalize_kernel(idx, *refs):
    xs, gains = refs[:8], refs[8:16]
    mod, normed, inv_out = refs[16:]
    rows = mod.shape[0]
    squares = jnp.zeros((rows, 256), F32)
    for a in xs:
        for s in range(2):
            xb = a[s].astype(F32)
            squares = squares + xb * xb
    inv = lax.rsqrt(jnp.sum(squares, axis=1, keepdims=True) / 4096 + epsilon)
    inv_out[...] = inv
    second = mod[...] == 1
    for n in range(16):
        a, s = n // 2, n % 2
        g = gains[a][s].astype(F32)
        g0 = (g[0:1] + g[2:3]) + g[4:5]
        g1 = (g[1:2] + g[3:4]) + g[5:6]
        scaled = xs[a][s].astype(F32) * inv
        normed[idx[n]] = (scaled * jnp.where(second, g1, g0)).astype(BF16)


def normalize(idx, xs, modality):
    tile = 128
    rows = lambda cols: pl.BlockSpec((tile, cols), lambda i: (i, 0))
    return pl.pallas_call(
        normalize_kernel,
        name="normalize",
        grid=(512 // tile,),
        in_specs=[SMEM]
        + [pl.BlockSpec((2, tile, 256), lambda i: (0, i, 0))] * 8
        + [pl.BlockSpec((2, 16, 256), lambda i: (0, 32, 0))] * 8
        + [rows(1)],
        out_specs=[pl.BlockSpec((16, tile, 256), lambda i: (0, i, 0)), rows(1)],
        out_shape=[shape((16, 512, 256)), shape((512, 1), F32)],
        compiler_params=PARAMS,
    )(idx, *xs, *xs, modality[:, None])


def project_kernel(normed, w, q, kv, kv_copies, acc):
    step = pl.program_id(0)
    total = dot(normed[0], w[0], NT)
    for k in range(1, 8):
        total = total + dot(normed[k], w[k], NT)

    @pl.when(step == 0)
    def _():
        acc[...] = total

    @pl.when(step == 1)
    def _():
        both = (acc[...] + total).astype(BF16)
        q[...] = both[:, 0:128]
        kv[...] = both[:, 128:384]
        for k in range(8):
            kv_copies[k] = both[:, 128:384]


def project(normed, w_t):
    return pl.pallas_call(
        project_kernel,
        name="project",
        grid=(2,),
        in_specs=[
            pl.BlockSpec((8, 512, 256), lambda j: (j, 0, 0)),
            pl.BlockSpec((8, 384, 256), lambda j: (j, 0, 0)),
        ],
        out_specs=[fixed(512, 128), fixed(512, 256), fixed(8, 512, 256)],
        out_shape=[shape((512, 128)), shape((512, 256)), shape((8, 512, 256))],
        scratch_shapes=[pltpu.VMEM((512, 384), F32)],
        compiler_params=PARAMS,
    )(normed, w_t)


def upstream_kernel(idx, *refs):
    gs, w, out, ordered = refs[:8], refs[8], refs[9], refs[10]
    acc = jnp.zeros(out.shape, F32)
    for n in range(16):
        g = gs[n // 2][n % 2]
        ordered[idx[n]] = g
        acc = acc + dot(g, w[idx[n]], NT)
    out[...] = acc.astype(BF16)


def upstream(idx, gs, wo):
    tile = 128
    return pl.pallas_call(
        upstream_kernel,
        name="upstream",
        grid=(512 // tile,),
        in_specs=[SMEM]
        + [pl.BlockSpec((2, tile, 256), lambda i: (0, i, 0))] * 8
        + [fixed(16, 128, 256)],
        out_specs=[
            pl.BlockSpec((tile, 128), lambda i: (i, 0)),
            pl.BlockSpec((16, tile, 256), lambda i: (0, i, 0)),
        ],
        out_shape=[shape((512, 128)), shape((16, 512, 256))],
        compiler_params=PARAMS,
    )(idx, *gs, wo)


KEY_BLOCK = 512
SCALE = 1.0 / math.sqrt(128)
TO_BASE2 = SCALE * math.log2(math.e)


def masked_scores(b, kv, q, edge):
    s = dot(kv[pl.ds(b * KEY_BLOCK, KEY_BLOCK), 0:128], q[...], NT) * TO_BASE2
    pos = lax.broadcasted_iota(jnp.int32, s.shape, 0) + b * KEY_BLOCK
    return jnp.where(pos < edge, s, masked_low)


def forward_kernel(limit, q, kv, att, att_t, lse, s_all):
    count = kv.shape[0] // KEY_BLOCK
    cols = q.shape[0]
    edge = limit[...]

    def scores(b, top):
        s = masked_scores(b, kv, q, edge)
        s_all[pl.ds(b * KEY_BLOCK, KEY_BLOCK), :] = s
        return jnp.maximum(top, jnp.max(s, axis=0, keepdims=True))

    top = lax.fori_loop(0, count, scores, jnp.full((1, cols), masked_low, F32))

    def sums(b, total):
        at = pl.ds(b * KEY_BLOCK, KEY_BLOCK)
        e = jnp.exp2(s_all[at, :] - top)
        s_all[at, :] = e
        return total + jnp.sum(e, axis=0, keepdims=True)

    total = lax.fori_loop(0, count, sums, jnp.zeros((1, cols), F32))
    inv = 1.0 / total
    lse[...] = top + jnp.log2(total)

    def attend(b, acc):
        at = pl.ds(b * KEY_BLOCK, KEY_BLOCK)
        return acc + dot(kv[at, 128:256], (s_all[at, :] * inv).astype(BF16), TN)

    out_t = lax.fori_loop(0, count, attend, jnp.zeros((128, cols), F32)).astype(BF16)
    att_t[...] = out_t
    att[...] = out_t.T


def forward(limit, q, kv):
    return pl.pallas_call(
        forward_kernel,
        name="forward",
        out_shape=[shape((512, 128)), shape((128, 512)), shape((1, 512), F32)],
        scratch_shapes=[pltpu.VMEM((4096, 512), F32)],
        compiler_params=PARAMS,
    )(limit, q, kv)


def backward_kernel(limit, lse, q, kv, da, att_t, dq, dkv):
    count = kv.shape[0] // KEY_BLOCK
    edge = limit[...]
    da_t = da[...].T
    row_dots = jnp.sum(att_t[...].astype(F32) * da_t.astype(F32), axis=0, keepdims=True)

    def back(b, acc):
        at = pl.ds(b * KEY_BLOCK, KEY_BLOCK)
        p = jnp.exp2(masked_scores(b, kv, q, edge) - lse[...])
        d_probs = dot(kv[at, 128:256], da[...], NT)
        ds = (p * (d_probs - row_dots) * SCALE).astype(BF16)
        dkv[at, 0:128] = dot(ds, q[...]).astype(BF16)
        dkv[at, 128:256] = dot(p.astype(BF16), da[...]).astype(BF16)
        return acc + dot(kv[at, 0:128], ds, TN)

    dq_t = lax.fori_loop(0, count, back, jnp.zeros((128, q.shape[0]), F32))
    dq[...] = dq_t.astype(BF16).T


def backward(limit, lse, q, kv, da, att_t):
    return pl.pallas_call(
        backward_kernel,
        name="backward",
        out_shape=[shape((512, 128)), shape((4096, 256))],
        compiler_params=PARAMS,
    )(limit, lse, q, kv, da, att_t)


def split_rows(dots):
    rows = []
    for p in (dots[:, 0:256], dots[:, 256:512]):
        high = p.astype(BF16).astype(F32)
        mid = (p - high).astype(BF16).astype(F32)
        rows.append((high, mid, p - high - mid))
    kind = lax.broadcasted_iota(jnp.int32, (16, 256), 0)
    both = jnp.zeros((16, 256), F32)
    for r in range(6):
        both = jnp.where(kind == r, rows[r % 2][r // 2], both)
    return both.astype(BF16)


def joined_rows(block):
    t = block.astype(F32)
    return (t[0:2] + t[2:4]) + t[4:6]


def collect_kernel(dkv, dq, q, kv, g_out, g_t, dots):
    total = dkv[0].astype(F32)
    for k in range(1, 8):
        total = total + dkv[k].astype(F32)
    g = jnp.concatenate([dq[...], total.astype(BF16)], axis=1)
    g_out[...] = g
    g_t[...] = g.T
    gf = g.astype(F32)
    prod = gf[:, 0:128] * q[...].astype(F32)
    prod = prod + gf[:, 128:256] * kv[:, 0:128].astype(F32)
    prod = prod + gf[:, 256:384] * kv[:, 128:256].astype(F32)
    dots[...] = lax.dot_general(
        jnp.ones((8, 128), F32), prod, NT, precision=lax.Precision.HIGHEST, preferred_element_type=F32
    )


def collect(dkv, dq, q, kv):
    return pl.pallas_call(
        collect_kernel,
        name="collect",
        out_shape=[shape((512, 384)), shape((384, 512)), shape((8, 512), F32)],
        compiler_params=PARAMS,
    )(dkv, dq, q, kv)


def input_grad_kernel(idx, g, g2, w, w2, dots, dots2, *outs):
    rows = split_rows(dots[0:1] + dots2[0:1])
    for n in range(8):
        out, at = outs[n // 2], idx[n]
        both = dot(g[...], w[at]) + dot(g2[...], w2[at])
        out[n % 2, 0:512, :] = both.astype(BF16)
        out[n % 2, 512:528, :] = rows


def input_grad(idx, g, g2, w, w2, dots, dots2):
    vmem = pl.BlockSpec(memory_space=pltpu.VMEM)
    return pl.pallas_call(
        input_grad_kernel,
        name="input_grad",
        in_specs=[SMEM] + [vmem] * 6,
        out_shape=[shape((2, 528, 256))] * 4,
        compiler_params=PARAMS,
    )(idx, g, g2, w, w2, dots, dots2)


def weight_grad_kernel(left, right, out):
    for k in range(right.shape[0]):
        out[k] = dot(left[...], right[k]).astype(BF16)


def weight_grad(left, right):
    rows = left.shape[0]
    return pl.pallas_call(
        weight_grad_kernel,
        name="weight_grad",
        grid=(2,),
        in_specs=[fixed(rows, 512), pl.BlockSpec((8, 512, 256), lambda j: (j, 0, 0))],
        out_specs=pl.BlockSpec((8, rows, 256), lambda j: (j, 0, 0)),
        out_shape=shape((16, rows, 256)),
        compiler_params=PARAMS,
    )(left, right)


def add_up_kernel(*refs):
    terms, out = refs[:-1], refs[-1]
    total = terms[0][0, 0:512].astype(F32)
    dots = joined_rows(terms[0][0, 512:528])
    for t in terms[1:]:
        total = total + t[0, 0:512].astype(F32)
        dots = dots + joined_rows(t[0, 512:528])
    out[0:512] = total.astype(BF16)
    out[512:528] = split_rows(jnp.concatenate([dots[0:1], dots[1:2]], axis=1))


def add_up(terms):
    return pl.pallas_call(
        add_up_kernel,
        name="add_up",
        grid=(1,),
        in_specs=[pl.BlockSpec((1, 528, 256), lambda i: (1, 0, 0))] * len(terms),
        out_specs=fixed(528, 256),
        out_shape=shape((528, 256)),
        compiler_params=PARAMS,
    )(*terms)


def finish_kernel(*refs):
    terms, (last, x, inv, mod, gain, grad_in, local_gain) = refs[:4], refs[4:]
    gn = last[0:512].astype(F32)
    dots = joined_rows(last[512:528])
    for t in terms:
        gn = gn + t[0, 0:512].astype(F32)
        dots = dots + joined_rows(t[0, 512:528])
    columns = [jnp.broadcast_to(dots[r : r + 1], (128, 256)).T[:, 0:1] for r in range(2)]
    mean = jnp.concatenate(columns, axis=0) / 4096
    second = mod[...] == 1
    scaled = x[...].astype(F32) * inv[...]
    up = gn * jnp.where(second, gain[1:2], gain[0:1])
    grad_in[...] = (inv[...] * (up - scaled * mean)).astype(BF16)
    each = gn * scaled
    sums = [jnp.sum(jnp.where(second, b, a), axis=0, keepdims=True) for a, b in ((each, 0.0), (0.0, each))]
    for k in range(8):
        local_gain[k, 0:1] = sums[0]
        local_gain[k, 1:2] = sums[1]


def finish(terms, last, x, inv, modality, gain):
    return pl.pallas_call(
        finish_kernel,
        name="finish",
        grid=(1,),
        in_specs=[pl.BlockSpec((1, 528, 256), lambda i: (0, 0, 0))] * 4
        + [fixed(528, 256), fixed(512, 256), fixed(512, 1), fixed(512, 1), fixed(2, 256)],
        out_specs=[fixed(512, 256), fixed(8, 2, 256)],
        out_shape=[shape((512, 256)), shape((8, 2, 256), F32)],
        compiler_params=PARAMS,
    )(*terms, last, x, inv, modality[:, None], gain)


def output_kernel(idx, *refs):
    atts, rows, out = refs[:8], refs[8], refs[9]
    total = jnp.zeros(out.shape, F32)
    for n in range(16):
        total = total + dot(atts[n // 2][n % 2], rows[idx[n]]).astype(BF16).astype(F32)
    out[...] = total.astype(BF16)


def output(idx, atts, rows):
    tile = 128
    return pl.pallas_call(
        output_kernel,
        name="output",
        grid=(512 // tile,),
        in_specs=[SMEM]
        + [pl.BlockSpec((2, tile, 128), lambda i: (0, i, 0))] * 8
        + [fixed(16, 128, 256)],
        out_specs=pl.BlockSpec((tile, 256), lambda i: (i, 0)),
        out_shape=shape((512, 256)),
        compiler_params=PARAMS,
    )(idx, *atts, rows)


def sum_qkv_kernel(parts, out):
    total = parts[0, 0].astype(F32)
    for k in range(1, 8):
        total = total + parts[k, 0].astype(F32)
    for m in range(3):
        out[m] = total[m * 128 : (m + 1) * 128].T


def sum_qkv(parts):
    return pl.pallas_call(
        sum_qkv_kernel,
        name="sum_qkv",
        grid=(2,),
        in_specs=[pl.BlockSpec((8, 1, 384, 256), lambda s: (0, s, 0, 0))],
        out_specs=pl.BlockSpec((3, 256, 128), lambda s: (0, s, 0)),
        out_shape=shape((3, 512, 128), F32),
        compiler_params=PARAMS,
    )(parts)


def sum_out_kernel(parts, out):
    total = parts[0].astype(F32)
    for k in range(1, 8):
        total = total + parts[k].astype(F32)
    out[:, 0:256] = total[0]
    out[:, 256:512] = total[1]


def sum_out(parts):
    return pl.pallas_call(
        sum_out_kernel,
        name="sum_out",
        out_shape=shape((128, 512), F32),
        compiler_params=PARAMS,
    )(parts)


def sublayer(layer_input, modality, image_spans, norm_gain, w_qkv, w_out, grad_out):
    x, h, c = (lax.axis_index(a) for a in GROUP)
    blocks = [((x - d) % 4, h ^ s, c ^ k) for k in range(2) for d in TURNS for s in range(2)]
    idx = jnp.stack([a * 4 + b * 2 + e for a, b, e in blocks]).astype(jnp.int32)
    places = jnp.stack([((x + d) % 4) * 2 + (h ^ s) for d in range(4) for s in range(2)]).astype(jnp.int32)

    gain_rows = jnp.concatenate(three_parts(norm_gain), axis=0).astype(BF16)
    gain_rows = jnp.concatenate([gain_rows, jnp.zeros((10, 256), BF16)], axis=0)
    xs = spread(jnp.concatenate([layer_input, gain_rows], axis=0))
    gs = spread(grad_out)

    w_t = exchange(pack_weights(w_qkv), TOKENS_AXES).reshape(16, 384, 256)
    wo_half = jnp.stack([w_out[:, 0:256], w_out[:, 256:512]])
    wo = exchange(copies(wo_half, 8), TOKENS_AXES).reshape(16, 128, 256)

    normed, inv = normalize(idx, xs, modality)
    q, kv, kv_copies = project(normed, w_t)
    all_kv = exchange(kv_copies, TOKENS_AXES).reshape(4096, 256)
    da, g_all = upstream(idx, gs, wo)
    w_pairs = w_t.reshape(8, 2, 384, 256)
    w_kept = lax.dynamic_index_in_dim(w_pairs, c, 1, keepdims=False)
    w_sent = lax.dynamic_index_in_dim(w_pairs, 1 - c, 1, keepdims=False)
    w_other = swap(w_sent, "c")

    pos = lax.axis_index(TOKENS_AXES) * 512 + jnp.arange(512, dtype=jnp.int32)
    inside = (pos[:, None] >= image_spans[0][None]) & (pos[:, None] < image_spans[1][None])
    ends = jnp.max(jnp.where(inside, image_spans[1][None], 0), axis=1)
    limit = jnp.maximum(pos + 1, ends)[None, :]

    out_rows = exchange(wo, GROUP)
    att, att_t, lse = forward(limit, q, all_kv)
    wo_parts = weight_grad(att_t, g_all).reshape(8, 2, 128, 256)
    wo_parts = exchange(wo_parts, TOKENS_AXES)
    dq, dkv = backward(limit, lse, q, all_kv, da, att_t)
    dkv_parts = exchange(dkv.reshape(8, 512, 256), TOKENS_AXES)

    atts = spread(att)
    attn_out = output(idx, atts, out_rows)
    grad_wout = sum_out(wo_parts)

    g, g_t, dots = collect(dkv_parts, dq, q, kv)
    g2, dots2 = swap(g, "c"), swap(dots, "c")
    w_parts = weight_grad(g_t, normed).reshape(8, 2, 384, 256)
    w_parts = exchange(w_parts, TOKENS_AXES)
    terms = input_grad(places, g, g2, w_kept, w_other, dots, dots2)
    terms = [turn(t, d) if d else t for d, t in enumerate(terms)]
    line = add_up(terms)
    last = swap(line, "h")
    grad_in, local_gain = finish(terms, last, layer_input, inv, modality, norm_gain)
    grad_qkv = sum_qkv(w_parts)
    grad_gain = jnp.sum(exchange(local_gain, TOKENS_AXES), axis=0)
    return (attn_out, grad_in, grad_qkv, grad_wout, grad_gain)


def solution(mesh):
    fine = Mesh(mesh.devices.reshape(4, 2, 2, 4, 2), ("x", "h", "c", "z", "u"))
    tok, feat = TOKENS_AXES, GROUP
    in_specs = (P(tok, feat), P(tok), P(), P(None, feat), P(None, tok, feat), P(feat, tok), P(tok, feat))
    out_specs = (P(tok, feat), P(tok, feat), P(None, tok, feat), P(feat, tok), P(None, feat))
    return jax.shard_map(sublayer, mesh=fine, in_specs=in_specs, out_specs=out_specs, check_vma=False)
```

```python
import math

import jax
import jax.numpy as jnp
from jax import lax
from jax.experimental import pallas as pl
from jax.experimental.pallas import tpu as pltpu
from jax.sharding import Mesh
from jax.sharding import PartitionSpec as P


epsilon = 1e-05
masked_low = -1e30
GROUP = ("x", "h", "c")
TOKENS_AXES = ("z", "u")
F32 = jnp.float32
BF16 = jnp.bfloat16
TURNS = (0, 1, 3, 2)
NT = (((1,), (1,)), ((), ()))
TN = (((0,), (0,)), ((), ()))
SMEM = pl.BlockSpec(memory_space=pltpu.SMEM)
PARAMS = pltpu.CompilerParams(vmem_limit_bytes=60 * 1024 * 1024)


def swap(a, axis):
    return lax.ppermute(a, axis, [(0, 1), (1, 0)])


def turn(a, d, axis="x"):
    return lax.ppermute(a, axis, [(i, (i + d) % 4) for i in range(4)])


def turns(a, axis="x"):
    return [a] + [turn(a, d, axis) for d in TURNS[1:]]


def spread(block):
    row = turns(block) + turns(swap(block, "h"))
    return row + [swap(a, "c") for a in row]


def gather_tokens_axes(block):
    return turns(block, "z") + turns(swap(block, "u"), "z")


def exchange(blocks, axis):
    return lax.all_to_all(blocks, axis, 0, 0, tiled=True)


def three_parts(g):
    high = lax.reduce_precision(g, 8, 7)
    rest = g - high
    mid = lax.reduce_precision(rest, 8, 7)
    return high, mid, rest - mid


def dot(a, b, dims=(((1,), (0,)), ((), ()))):
    return lax.dot_general(a, b, dims, preferred_element_type=F32)


def shape(dims, kind=BF16):
    return jax.ShapeDtypeStruct(dims, kind)


def fixed(*dims):
    return pl.BlockSpec(dims, lambda *i: (0,) * len(dims))


def pack_kernel(w, wo, out):
    for s in range(2):
        for m in range(3):
            out[s, m * 128 : (m + 1) * 128, :] = w[m, s * 256 : (s + 1) * 256, :].T
        out[s, 384:512, :] = wo[:, s * 256 : (s + 1) * 256]


def pack_weights(w, wo):
    return pl.pallas_call(
        pack_kernel,
        name="pack_weights",
        out_shape=shape((2, 512, 256)),
        compiler_params=PARAMS,
    )(w, wo)


def normalize_kernel(idx, *refs):
    xs, gains = refs[:16], refs[16:32]
    mod, normed, inv_out = refs[32:]
    rows = mod.shape[0]
    squares = jnp.zeros((rows, 256), F32)
    for a in xs:
        xb = a[...].astype(F32)
        squares = squares + xb * xb
    inv = lax.rsqrt(jnp.sum(squares, axis=1, keepdims=True) / 4096 + epsilon)
    inv_out[...] = inv
    second = mod[...] == 1
    for n in range(16):
        g = gains[n][...].astype(F32)
        g0 = (g[0:1] + g[2:3]) + g[4:5]
        g1 = (g[1:2] + g[3:4]) + g[5:6]
        scaled = xs[n][...].astype(F32) * inv
        normed[idx[n]] = (scaled * jnp.where(second, g1, g0)).astype(BF16)


def normalize(idx, xs, modality):
    tile = 128
    rows = lambda cols: pl.BlockSpec((tile, cols), lambda i: (i, 0))
    return pl.pallas_call(
        normalize_kernel,
        name="normalize",
        grid=(512 // tile,),
        in_specs=[SMEM] + [rows(256)] * 16 + [pl.BlockSpec((16, 256), lambda i: (32, 0))] * 16 + [rows(1)],
        out_specs=[pl.BlockSpec((16, tile, 256), lambda i: (0, i, 0)), rows(1)],
        out_shape=[shape((16, 512, 256)), shape((512, 1), F32)],
        compiler_params=PARAMS,
    )(idx, *xs, *xs, modality[:, None])


def project_kernel(idx, normed, *refs):
    ws, (q, kv) = refs[:8], refs[8:]
    total = jnp.zeros((q.shape[0], 384), F32)
    for n in range(8):
        for s in range(2):
            total = total + dot(normed[idx[n] * 2 + s], ws[n][s], NT)
    both = total.astype(BF16)
    q[...] = both[:, 0:128]
    kv[...] = both[:, 128:384]


def project(idx, normed, ws):
    tile = 256
    rows = lambda cols: pl.BlockSpec((tile, cols), lambda i: (i, 0))
    return pl.pallas_call(
        project_kernel,
        name="project",
        grid=(512 // tile,),
        in_specs=[SMEM, pl.BlockSpec((16, tile, 256), lambda i: (0, i, 0))] + [fixed(2, 384, 256)] * 8,
        out_specs=[rows(128), rows(256)],
        out_shape=[shape((512, 128)), shape((512, 256))],
        compiler_params=PARAMS,
    )(idx, normed, *ws)


def order_kernel(idx, core, *refs):
    ws, (kept, sent, wo) = refs[:8], refs[8:]
    for n in range(8):
        k = idx[n]
        kept[k] = ws[n][core[0], 0:384, :]
        sent[k] = ws[n][1 - core[0], 0:384, :]
        for s in range(2):
            wo[k * 2 + s] = ws[n][s, 384:512, :]


def order_weights(idx, core, ws):
    vmem = pl.BlockSpec(memory_space=pltpu.VMEM)
    return pl.pallas_call(
        order_kernel,
        name="order_weights",
        in_specs=[SMEM, SMEM] + [vmem] * 8,
        out_shape=[shape((8, 384, 256)), shape((8, 384, 256)), shape((16, 128, 256))],
        compiler_params=PARAMS,
    )(idx, core, *ws)


def upstream_kernel(idx, *refs):
    gs, (w, out, ordered) = refs[:16], refs[16:]
    acc = jnp.zeros(out.shape, F32)
    for n in range(16):
        g = gs[n][...]
        ordered[idx[n]] = g
        acc = acc + dot(g, w[idx[n]], NT)
    out[...] = acc.astype(BF16)


def upstream(idx, gs, wo):
    tile = 128
    return pl.pallas_call(
        upstream_kernel,
        name="upstream",
        grid=(512 // tile,),
        in_specs=[SMEM]
        + [pl.BlockSpec((tile, 256), lambda i: (i, 0))] * 16
        + [fixed(16, 128, 256)],
        out_specs=[
            pl.BlockSpec((tile, 128), lambda i: (i, 0)),
            pl.BlockSpec((16, tile, 256), lambda i: (0, i, 0)),
        ],
        out_shape=[shape((512, 128)), shape((16, 512, 256))],
        compiler_params=PARAMS,
    )(idx, *gs, wo)


KEY_BLOCK = 512
SCALE = 1.0 / math.sqrt(128)
TO_BASE2 = SCALE * math.log2(math.e)


def masked_scores(b, kv, q, edge):
    s = dot(kv[pl.ds(b * KEY_BLOCK, KEY_BLOCK), 0:128], q[...], NT) * TO_BASE2
    pos = lax.broadcasted_iota(jnp.int32, s.shape, 0) + b * KEY_BLOCK
    return jnp.where(pos < edge, s, masked_low)


def forward_kernel(idx, limit, q, *refs):
    parts, (att, att_t, lse, kv, s_all) = refs[:8], refs[8:]
    for n in range(8):
        kv[pl.ds(idx[n] * 512, 512), :] = parts[n][...]
    count = kv.shape[0] // KEY_BLOCK
    cols = q.shape[0]
    edge = limit[...]

    def scores(b, top):
        s = masked_scores(b, kv, q, edge)
        s_all[pl.ds(b * KEY_BLOCK, KEY_BLOCK), :] = s
        return jnp.maximum(top, jnp.max(s, axis=0, keepdims=True))

    top = lax.fori_loop(0, count, scores, jnp.full((1, cols), masked_low, F32))

    def sums(b, total):
        at = pl.ds(b * KEY_BLOCK, KEY_BLOCK)
        e = jnp.exp2(s_all[at, :] - top)
        s_all[at, :] = e
        return total + jnp.sum(e, axis=0, keepdims=True)

    total = lax.fori_loop(0, count, sums, jnp.zeros((1, cols), F32))
    inv = 1.0 / total
    lse[...] = top + jnp.log2(total)

    def attend(b, acc):
        at = pl.ds(b * KEY_BLOCK, KEY_BLOCK)
        return acc + dot(kv[at, 128:256], (s_all[at, :] * inv).astype(BF16), TN)

    out_t = lax.fori_loop(0, count, attend, jnp.zeros((128, cols), F32)).astype(BF16)
    att_t[...] = out_t
    att[...] = out_t.T


def forward(idx, limit, q, parts):
    vmem = pl.BlockSpec(memory_space=pltpu.VMEM)
    return pl.pallas_call(
        forward_kernel,
        name="forward",
        in_specs=[SMEM] + [vmem] * 10,
        out_shape=[shape((512, 128)), shape((128, 512)), shape((1, 512), F32), shape((4096, 256))],
        scratch_shapes=[pltpu.VMEM((4096, 512), F32)],
        compiler_params=PARAMS,
    )(idx, limit, q, *parts)


def backward_kernel(limit, lse, q, kv, da, att_t, dq, dkv):
    count = kv.shape[0] // KEY_BLOCK
    edge = limit[...]
    da_t = da[...].T
    row_dots = jnp.sum(att_t[...].astype(F32) * da_t.astype(F32), axis=0, keepdims=True)

    def back(b, acc):
        at = pl.ds(b * KEY_BLOCK, KEY_BLOCK)
        p = jnp.exp2(masked_scores(b, kv, q, edge) - lse[...])
        d_probs = dot(kv[at, 128:256], da[...], NT)
        ds = (p * (d_probs - row_dots) * SCALE).astype(BF16)
        dkv[at, 0:128] = dot(ds, q[...]).astype(BF16)
        dkv[at, 128:256] = dot(p.astype(BF16), da[...]).astype(BF16)
        return acc + dot(kv[at, 0:128], ds, TN)

    dq_t = lax.fori_loop(0, count, back, jnp.zeros((128, q.shape[0]), F32))
    dq[...] = dq_t.astype(BF16).T


def backward(limit, lse, q, kv, da, att_t):
    return pl.pallas_call(
        backward_kernel,
        name="backward",
        out_shape=[shape((512, 128)), shape((4096, 256))],
        compiler_params=PARAMS,
    )(limit, lse, q, kv, da, att_t)


def split_rows(dots):
    rows = []
    for p in (dots[:, 0:256], dots[:, 256:512]):
        high = p.astype(BF16).astype(F32)
        mid = (p - high).astype(BF16).astype(F32)
        rows.append((high, mid, p - high - mid))
    kind = lax.broadcasted_iota(jnp.int32, (16, 256), 0)
    both = jnp.zeros((16, 256), F32)
    for r in range(6):
        both = jnp.where(kind == r, rows[r % 2][r // 2], both)
    return both.astype(BF16)


def joined_rows(block):
    t = block.astype(F32)
    return (t[0:2] + t[2:4]) + t[4:6]


def gradients_kernel(dkv, dq, q, kv, normed, dwo, g_out, dots, out, g_t):
    step = pl.program_id(0)

    @pl.when(step == 0)
    def _():
        total = dkv[0].astype(F32)
        for k in range(1, 8):
            total = total + dkv[k].astype(F32)
        g = jnp.concatenate([dq[...], total.astype(BF16)], axis=1)
        g_out[...] = g
        g_t[...] = g.T
        gf = g.astype(F32)
        prod = gf[:, 0:128] * q[...].astype(F32)
        prod = prod + gf[:, 128:256] * kv[:, 0:128].astype(F32)
        prod = prod + gf[:, 256:384] * kv[:, 128:256].astype(F32)
        ones = jnp.ones((8, 128), F32)
        dots[...] = lax.dot_general(
            ones, prod, NT, precision=lax.Precision.HIGHEST, preferred_element_type=F32
        )

    @pl.when(step > 0)
    def _():
        for k in range(8):
            out[k, 0:384, :] = dot(g_t[...], normed[k]).astype(BF16)
            out[k, 384:512, :] = dwo[k]


def gradients(dkv, dq, q, kv, normed, dwo):
    later = lambda i: (jnp.maximum(i - 1, 0), 0, 0)
    return pl.pallas_call(
        gradients_kernel,
        name="gradients",
        grid=(3,),
        in_specs=[
            fixed(8, 512, 256),
            fixed(512, 128),
            fixed(512, 128),
            fixed(512, 256),
            pl.BlockSpec((8, 512, 256), later),
            pl.BlockSpec((8, 128, 256), later),
        ],
        out_specs=[fixed(512, 384), fixed(8, 512), pl.BlockSpec((8, 512, 256), later)],
        out_shape=[shape((512, 384)), shape((8, 512), F32), shape((16, 512, 256))],
        scratch_shapes=[pltpu.VMEM((384, 512), BF16)],
        compiler_params=PARAMS,
    )(dkv, dq, q, kv, normed, dwo)


def input_grad_kernel(idx, g, g2, w, w2, dots, dots2, *outs):
    rows = split_rows(dots[0:1] + dots2[0:1])
    for n in range(8):
        out, at = outs[n // 2], idx[n]
        both = dot(g[...], w[at]) + dot(g2[...], w2[at])
        out[n % 2, 0:512, :] = both.astype(BF16)
        out[n % 2, 512:528, :] = rows


def input_grad(idx, g, g2, w, w2, dots, dots2):
    vmem = pl.BlockSpec(memory_space=pltpu.VMEM)
    return pl.pallas_call(
        input_grad_kernel,
        name="input_grad",
        in_specs=[SMEM] + [vmem] * 6,
        out_shape=[shape((2, 528, 256))] * 4,
        compiler_params=PARAMS,
    )(idx, g, g2, w, w2, dots, dots2)


def weight_grad_kernel(left, right, out):
    for k in range(right.shape[0]):
        out[k] = dot(left[...], right[k]).astype(BF16)


def weight_grad(left, right):
    rows = left.shape[0]
    return pl.pallas_call(
        weight_grad_kernel,
        name="weight_grad",
        grid=(2,),
        in_specs=[fixed(rows, 512), pl.BlockSpec((8, 512, 256), lambda j: (j, 0, 0))],
        out_specs=pl.BlockSpec((8, rows, 256), lambda j: (j, 0, 0)),
        out_shape=shape((16, rows, 256)),
        compiler_params=PARAMS,
    )(left, right)


def line_kernel(side, *refs):
    terms, (x, x_next, inv, mod, own, own_dots, sent, gains) = refs[:4], refs[4:]
    second = mod[...] == 1
    for slot, block in ((0, x), (1, x_next)):
        total = terms[0][slot, 0:512].astype(F32)
        dots = joined_rows(terms[0][slot, 512:528])
        for t in terms[1:]:
            total = total + t[slot, 0:512].astype(F32)
            dots = dots + joined_rows(t[slot, 512:528])
        if slot == 0:
            own[...] = total
            own_dots[0:2] = dots
        else:
            sent[0:512] = total.astype(BF16)
            sent[512:528] = split_rows(jnp.concatenate([dots[0:1], dots[1:2]], axis=1))
        each = total * (block[...].astype(F32) * inv[...])
        first = jnp.sum(jnp.where(second, 0.0, each), axis=0, keepdims=True)
        other = jnp.sum(jnp.where(second, each, 0.0), axis=0, keepdims=True)
        at = side[0] if slot == 0 else 1 - side[0]
        for k in range(8):
            gains[k, at, 0:1] = first
            gains[k, at, 1:2] = other


def line_sum(side, terms, x, x_next, inv, modality):
    return pl.pallas_call(
        line_kernel,
        name="line_sum",
        grid=(1,),
        in_specs=[SMEM]
        + [fixed(2, 528, 256)] * 4
        + [fixed(512, 256), fixed(512, 256), fixed(512, 1), fixed(512, 1)],
        out_specs=[fixed(512, 256), fixed(8, 256), fixed(528, 256), fixed(8, 2, 2, 256)],
        out_shape=[
            shape((512, 256), F32),
            shape((8, 256), F32),
            shape((528, 256)),
            shape((8, 2, 2, 256), F32),
        ],
        compiler_params=PARAMS,
    )(side, *terms, x, x_next, inv, modality[:, None])


def finish_kernel(own, own_dots, last, x, inv, mod, gain, grad_in):
    gn = own[...] + last[0:512].astype(F32)
    dots = own_dots[0:2] + joined_rows(last[512:528])
    columns = [jnp.broadcast_to(dots[r : r + 1], (128, 256)).T[:, 0:1] for r in range(2)]
    mean = jnp.concatenate(columns, axis=0) / 4096
    scaled = x[...].astype(F32) * inv[...]
    up = gn * jnp.where(mod[...] == 1, gain[1:2], gain[0:1])
    grad_in[...] = (inv[...] * (up - scaled * mean)).astype(BF16)


def finish(own, own_dots, last, x, inv, modality, gain):
    return pl.pallas_call(
        finish_kernel,
        name="finish",
        out_shape=shape((512, 256)),
        compiler_params=PARAMS,
    )(own, own_dots, last, x, inv, modality[:, None], gain)


def output_kernel(idx, *refs):
    atts, (rows, out) = refs[:16], refs[16:]
    total = jnp.zeros(out.shape, F32)
    for n in range(16):
        total = total + dot(atts[n][...], rows[idx[n]]).astype(BF16).astype(F32)
    out[...] = total.astype(BF16)


def output(idx, atts, rows):
    tile = 128
    return pl.pallas_call(
        output_kernel,
        name="output",
        grid=(512 // tile,),
        in_specs=[SMEM]
        + [pl.BlockSpec((tile, 128), lambda i: (i, 0))] * 16
        + [fixed(16, 128, 256)],
        out_specs=pl.BlockSpec((tile, 256), lambda i: (i, 0)),
        out_shape=shape((512, 256)),
        compiler_params=PARAMS,
    )(idx, *atts, rows)


def sum_weights_kernel(parts, qkv, wout):
    total = parts[0, 0].astype(F32)
    for k in range(1, 8):
        total = total + parts[k, 0].astype(F32)
    for m in range(3):
        qkv[m] = total[m * 128 : (m + 1) * 128].T
    wout[...] = total[384:512]


def sum_weights(parts):
    return pl.pallas_call(
        sum_weights_kernel,
        name="sum_weights",
        grid=(2,),
        in_specs=[pl.BlockSpec((8, 1, 512, 256), lambda s: (0, s, 0, 0))],
        out_specs=[
            pl.BlockSpec((3, 256, 128), lambda s: (0, s, 0)),
            pl.BlockSpec((128, 256), lambda s: (0, s)),
        ],
        out_shape=[shape((3, 512, 128), F32), shape((128, 512), F32)],
        compiler_params=PARAMS,
    )(parts)


def sublayer(layer_input, modality, image_spans, norm_gain, w_qkv, w_out, grad_out):
    x, h, c = (lax.axis_index(a) for a in GROUP)
    z, u = (lax.axis_index(a) for a in TOKENS_AXES)
    blocks = [((x - d) % 4, h ^ s, c ^ k) for k in range(2) for s in range(2) for d in TURNS]
    idx = jnp.stack([a * 4 + b * 2 + e for a, b, e in blocks]).astype(jnp.int32)
    tok_idx = jnp.stack([((z - d) % 4) * 2 + (u ^ s) for s in range(2) for d in TURNS]).astype(jnp.int32)
    places = jnp.stack([((x + d) % 4) * 2 + (h ^ s) for d in range(4) for s in range(2)]).astype(jnp.int32)
    core = c.astype(jnp.int32)[None]
    side = h.astype(jnp.int32)[None]

    gain_rows = jnp.concatenate(three_parts(norm_gain), axis=0).astype(BF16)
    gain_rows = jnp.concatenate([gain_rows, jnp.zeros((10, 256), BF16)], axis=0)
    xs = spread(jnp.concatenate([layer_input, gain_rows], axis=0))
    ws = gather_tokens_axes(pack_weights(w_qkv, w_out))
    gs = spread(grad_out)

    normed, inv = normalize(idx, xs, modality)
    q, kv = project(tok_idx, normed, ws)
    kvs = gather_tokens_axes(kv)
    w_kept, w_sent, wo = order_weights(tok_idx, core, ws)
    w_other = swap(w_sent, "c")
    da, g_all = upstream(idx, gs, wo)

    pos = (z * 2 + u) * 512 + jnp.arange(512, dtype=jnp.int32)
    inside = (pos[:, None] >= image_spans[0][None]) & (pos[:, None] < image_spans[1][None])
    ends = jnp.max(jnp.where(inside, image_spans[1][None], 0), axis=1)
    limit = jnp.maximum(pos + 1, ends)[None, :]

    out_rows = exchange(wo, GROUP)
    att, att_t, lse, all_kv = forward(tok_idx, limit, q, kvs)
    dq, dkv = backward(limit, lse, q, all_kv, da, att_t)
    dkv_parts = exchange(dkv.reshape(8, 512, 256), TOKENS_AXES)

    dwo = weight_grad(att_t, g_all)
    atts = spread(att)
    attn_out = output(idx, atts, out_rows)

    g, dots, w_parts = gradients(dkv_parts, dq, q, kv, normed, dwo)
    w_parts = exchange(w_parts.reshape(8, 2, 512, 256), TOKENS_AXES)
    g2, dots2 = swap(g, "c"), swap(dots, "c")
    terms = input_grad(places, g, g2, w_kept, w_other, dots, dots2)
    terms = [turn(t, d) if d else t for d, t in enumerate(terms)]
    own, own_dots, sent, gains = line_sum(side, terms, layer_input, xs[4], inv, modality)
    last = swap(sent, "h")
    gains = exchange(gains.reshape(16, 2, 256), ("z", "u", "h"))
    grad_in = finish(own, own_dots, last, layer_input, inv, modality, norm_gain)
    grad_qkv, grad_wout = sum_weights(w_parts)
    grad_gain = jnp.sum(gains, axis=0)
    return (attn_out, grad_in, grad_qkv, grad_wout, grad_gain)


def solution(mesh):
    fine = Mesh(mesh.devices.reshape(4, 2, 2, 4, 2), ("x", "h", "c", "z", "u"))
    tok, feat = TOKENS_AXES, GROUP
    in_specs = (P(tok, feat), P(tok), P(), P(None, feat), P(None, tok, feat), P(feat, tok), P(tok, feat))
    out_specs = (P(tok, feat), P(tok, feat), P(None, tok, feat), P(feat, tok), P(None, feat))
    return jax.shard_map(sublayer, mesh=fine, in_specs=in_specs, out_specs=out_specs, check_vma=False)
```

```python
import math

import jax
import jax.numpy as jnp
from jax import lax
from jax.experimental import pallas as pl
from jax.experimental.pallas import tpu as pltpu
from jax.sharding import Mesh
from jax.sharding import PartitionSpec as P


epsilon = 1e-05
masked_low = -1e30
GROUP = ("x", "h", "c")
TOKENS_AXES = ("z", "u")
F32 = jnp.float32
BF16 = jnp.bfloat16
TURNS = (0, 1, 3, 2)
NT = (((1,), (1,)), ((), ()))
TN = (((0,), (0,)), ((), ()))
SMEM = pl.BlockSpec(memory_space=pltpu.SMEM)
PARAMS = pltpu.CompilerParams(vmem_limit_bytes=60 * 1024 * 1024)


def swap(a, axis):
    return lax.ppermute(a, axis, [(0, 1), (1, 0)])


def turn(a, d, axis="x"):
    return lax.ppermute(a, axis, [(i, (i + d) % 4) for i in range(4)])


def turns(a, axis="x"):
    return [a] + [turn(a, d, axis) for d in TURNS[1:]]


def spread(block):
    row = turns(block) + turns(swap(block, "h"))
    return row + [swap(a, "c") for a in row]


def gather_tokens_axes(block):
    own = [block] + [turn(block, d, "z") for d in (1, 3)]
    own.append(turn(block, 2, "z"))
    near = swap(block, "u")
    near = [near] + [turn(near, d, "z") for d in (1, 3)]
    return own + near + [swap(own[3], "u")]


def exchange(blocks, axis):
    return lax.all_to_all(blocks, axis, 0, 0, tiled=True)


def three_parts(g):
    high = lax.reduce_precision(g, 8, 7)
    rest = g - high
    mid = lax.reduce_precision(rest, 8, 7)
    return high, mid, rest - mid


def dot(a, b, dims=(((1,), (0,)), ((), ()))):
    return lax.dot_general(a, b, dims, preferred_element_type=F32)


def shape(dims, kind=BF16):
    return jax.ShapeDtypeStruct(dims, kind)


def fixed(*dims):
    return pl.BlockSpec(dims, lambda *i: (0,) * len(dims))


def pack_kernel(w, wo, out):
    for s in range(2):
        for m in range(3):
            out[s, m * 128 : (m + 1) * 128, :] = w[m, s * 256 : (s + 1) * 256, :].T
        out[s, 384:512, :] = wo[:, s * 256 : (s + 1) * 256]


def pack_weights(w, wo):
    return pl.pallas_call(
        pack_kernel,
        name="pack_weights",
        out_shape=shape((2, 512, 256)),
        compiler_params=PARAMS,
    )(w, wo)


def normalize_kernel(idx, *refs):
    xs, gains = refs[:16], refs[16:32]
    mod, normed, inv_out = refs[32:]
    rows = mod.shape[0]
    squares = jnp.zeros((rows, 256), F32)
    for a in xs:
        xb = a[...].astype(F32)
        squares = squares + xb * xb
    inv = lax.rsqrt(jnp.sum(squares, axis=1, keepdims=True) / 4096 + epsilon)
    inv_out[...] = inv
    second = mod[...] == 1
    for n in range(16):
        g = gains[n][...].astype(F32)
        g0 = (g[0:1] + g[2:3]) + g[4:5]
        g1 = (g[1:2] + g[3:4]) + g[5:6]
        scaled = xs[n][...].astype(F32) * inv
        normed[idx[n]] = (scaled * jnp.where(second, g1, g0)).astype(BF16)


def normalize(idx, xs, modality):
    tile = 128
    rows = lambda cols: pl.BlockSpec((tile, cols), lambda i: (i, 0))
    return pl.pallas_call(
        normalize_kernel,
        name="normalize",
        grid=(512 // tile,),
        in_specs=[SMEM] + [rows(256)] * 16 + [pl.BlockSpec((16, 256), lambda i: (32, 0))] * 16 + [rows(1)],
        out_specs=[pl.BlockSpec((16, tile, 256), lambda i: (0, i, 0)), rows(1)],
        out_shape=[shape((16, 512, 256)), shape((512, 1), F32)],
        compiler_params=PARAMS,
    )(idx, *xs, *xs, modality)


def project_kernel(idx, normed, *refs):
    ws, (q, kv) = refs[:8], refs[8:]
    total = jnp.zeros((q.shape[0], 384), F32)
    for n in range(8):
        for s in range(2):
            total = total + dot(normed[idx[n] * 2 + s], ws[n][s], NT)
    both = total.astype(BF16)
    q[...] = both[:, 0:128]
    kv[...] = both[:, 128:384]


def project(idx, normed, ws):
    tile = 256
    rows = lambda cols: pl.BlockSpec((tile, cols), lambda i: (i, 0))
    return pl.pallas_call(
        project_kernel,
        name="project",
        grid=(512 // tile,),
        in_specs=[SMEM, pl.BlockSpec((16, tile, 256), lambda i: (0, i, 0))] + [fixed(2, 384, 256)] * 8,
        out_specs=[rows(128), rows(256)],
        out_shape=[shape((512, 128)), shape((512, 256))],
        compiler_params=PARAMS,
    )(idx, normed, *ws)


def order_kernel(idx, core, *refs):
    ws, (kept, sent) = refs[:8], refs[8:]
    for n in range(8):
        k = idx[n]
        kept[k] = ws[n][core[0]]
        sent[k] = ws[n][1 - core[0]]


def order_weights(idx, core, ws):
    return pl.pallas_call(
        order_kernel,
        name="order_weights",
        grid=(1,),
        in_specs=[SMEM, SMEM] + [fixed(2, 384, 256)] * 8,
        out_specs=[fixed(8, 384, 256)] * 2,
        out_shape=[shape((8, 384, 256))] * 2,
        compiler_params=PARAMS,
    )(idx, core, *ws)


def upstream_kernel(idx, tok_idx, *refs):
    gs, ws, (out, ordered, wo) = refs[:16], refs[16:24], refs[24:]

    @pl.when(pl.program_id(0) == 0)
    def _():
        for n in range(8):
            for s in range(2):
                wo[tok_idx[n] * 2 + s] = ws[n][s]

    acc = jnp.zeros(out.shape, F32)
    for n in range(16):
        g = gs[n][...]
        ordered[idx[n]] = g
        acc = acc + dot(g, wo[idx[n]], NT)
    out[...] = acc.astype(BF16)


def upstream(idx, tok_idx, gs, ws):
    tile = 128
    return pl.pallas_call(
        upstream_kernel,
        name="upstream",
        grid=(512 // tile,),
        in_specs=[SMEM, SMEM]
        + [pl.BlockSpec((tile, 256), lambda i: (i, 0))] * 16
        + [pl.BlockSpec((2, 128, 256), lambda i: (0, 3, 0))] * 8,
        out_specs=[
            pl.BlockSpec((tile, 128), lambda i: (i, 0)),
            pl.BlockSpec((16, tile, 256), lambda i: (0, i, 0)),
            fixed(16, 128, 256),
        ],
        out_shape=[shape((512, 128)), shape((16, 512, 256)), shape((16, 128, 256))],
        compiler_params=PARAMS,
    )(idx, tok_idx, *gs, *ws)


KEY_BLOCK = 512
SCALE = 1.0 / math.sqrt(128)
TO_BASE2 = SCALE * math.log2(math.e)


def masked_scores(b, kv, q, edge):
    s = dot(kv[pl.ds(b * KEY_BLOCK, KEY_BLOCK), 0:128], q[...], NT) * TO_BASE2
    pos = lax.broadcasted_iota(jnp.int32, s.shape, 0) + b * KEY_BLOCK
    return jnp.where(pos < edge, s, masked_low)


def forward_kernel(idx, limit, q, *refs):
    parts, (att, att_t, lse, kv, s_all) = refs[:8], refs[8:]
    for n in range(8):
        kv[pl.ds(idx[n] * 512, 512), :] = parts[n][...]
    count = kv.shape[0] // KEY_BLOCK
    cols = q.shape[0]
    edge = limit[...]

    def scores(b, top):
        s = masked_scores(b, kv, q, edge)
        s_all[pl.ds(b * KEY_BLOCK, KEY_BLOCK), :] = s
        return jnp.maximum(top, jnp.max(s, axis=0, keepdims=True))

    top = lax.fori_loop(0, count, scores, jnp.full((1, cols), masked_low, F32))

    def sums(b, total):
        at = pl.ds(b * KEY_BLOCK, KEY_BLOCK)
        e = jnp.exp2(s_all[at, :] - top)
        s_all[at, :] = e
        return total + jnp.sum(e, axis=0, keepdims=True)

    total = lax.fori_loop(0, count, sums, jnp.zeros((1, cols), F32))
    inv = 1.0 / total
    lse[...] = top + jnp.log2(total)

    def attend(b, acc):
        at = pl.ds(b * KEY_BLOCK, KEY_BLOCK)
        return acc + dot(kv[at, 128:256], (s_all[at, :] * inv).astype(BF16), TN)

    out_t = lax.fori_loop(0, count, attend, jnp.zeros((128, cols), F32)).astype(BF16)
    att_t[...] = out_t
    att[...] = out_t.T


def forward(idx, limit, q, parts):
    vmem = pl.BlockSpec(memory_space=pltpu.VMEM)
    return pl.pallas_call(
        forward_kernel,
        name="forward",
        in_specs=[SMEM] + [vmem] * 10,
        out_shape=[shape((512, 128)), shape((128, 512)), shape((1, 512), F32), shape((4096, 256))],
        scratch_shapes=[pltpu.VMEM((4096, 512), F32)],
        compiler_params=PARAMS,
    )(idx, limit, q, *parts)


def backward_kernel(limit, lse, q, kv, da, att_t, dq, dkv):
    count = kv.shape[0] // KEY_BLOCK
    edge = limit[...]
    da_t = da[...].T
    row_dots = jnp.sum(att_t[...].astype(F32) * da_t.astype(F32), axis=0, keepdims=True)

    def back(b, acc):
        at = pl.ds(b * KEY_BLOCK, KEY_BLOCK)
        p = jnp.exp2(masked_scores(b, kv, q, edge) - lse[...])
        d_probs = dot(kv[at, 128:256], da[...], NT)
        ds = (p * (d_probs - row_dots) * SCALE).astype(BF16)
        dkv[at, 0:128] = dot(ds, q[...]).astype(BF16)
        dkv[at, 128:256] = dot(p.astype(BF16), da[...]).astype(BF16)
        return acc + dot(kv[at, 0:128], ds, TN)

    dq_t = lax.fori_loop(0, count, back, jnp.zeros((128, q.shape[0]), F32))
    dq[...] = dq_t.astype(BF16).T


def backward(limit, lse, q, kv, da, att_t):
    return pl.pallas_call(
        backward_kernel,
        name="backward",
        out_shape=[shape((512, 128)), shape((4096, 256))],
        compiler_params=PARAMS,
    )(limit, lse, q, kv, da, att_t)


def split_rows(dots):
    rows = []
    for p in (dots[:, 0:256], dots[:, 256:512]):
        high = p.astype(BF16).astype(F32)
        mid = (p - high).astype(BF16).astype(F32)
        rows.append((high, mid, p - high - mid))
    kind = lax.broadcasted_iota(jnp.int32, (16, 256), 0)
    both = jnp.zeros((16, 256), F32)
    for r in range(6):
        both = jnp.where(kind == r, rows[r % 2][r // 2], both)
    return both.astype(BF16)


def joined_rows(block):
    t = block.astype(F32)
    return (t[0:2] + t[2:4]) + t[4:6]


def gradients_kernel(idx, dkv, dq, q, kv, n0, n1, w0, w1, g_out, dots, up, down, far, far_next, here, g_t):
    step = pl.program_id(0)

    @pl.when(step == 0)
    def _():
        total = dkv[0].astype(F32)
        for k in range(1, 8):
            total = total + dkv[k].astype(F32)
        g = jnp.concatenate([dq[...], total.astype(BF16)], axis=1)
        g_out[...] = g
        g_t[...] = g.T
        gf = g.astype(F32)
        prod = gf[:, 0:128] * q[...].astype(F32)
        prod = prod + gf[:, 128:256] * kv[:, 0:128].astype(F32)
        prod = prod + gf[:, 256:384] * kv[:, 128:256].astype(F32)
        ones = jnp.ones((8, 128), F32)
        dots[...] = lax.dot_general(
            ones, prod, NT, precision=lax.Precision.HIGHEST, preferred_element_type=F32
        )

    outs = ((up.at[0], up.at[1]), (down.at[0], down.at[1]), (far, far_next), (here.at[0], here.at[1]))
    for n, pair in enumerate(outs):

        @pl.when(step == n + 1)
        def _(pair=pair):
            for out, block, wo in ((pair[0], n0, w0), (pair[1], n1, w1)):
                for k in range(2):
                    out[k, 0:384, :] = dot(g_t[...], block[k]).astype(BF16)
                    out[k, 384:512, :] = wo[k]


def gradients(idx, dkv, dq, q, kv, normed, dwo):
    at = lambda slot: lambda i, idx: (idx[2 * jnp.maximum(i - 1, 0) + slot], 0, 0)
    spec = pltpu.PrefetchScalarGridSpec(
        num_scalar_prefetch=1,
        grid=(5,),
        in_specs=[
            fixed(8, 512, 256),
            fixed(512, 128),
            fixed(512, 128),
            fixed(512, 256),
            pl.BlockSpec((2, 512, 256), at(0)),
            pl.BlockSpec((2, 512, 256), at(1)),
            pl.BlockSpec((2, 128, 256), at(0)),
            pl.BlockSpec((2, 128, 256), at(1)),
        ],
        out_specs=[
            fixed(512, 384),
            fixed(8, 512),
            fixed(2, 2, 512, 256),
            fixed(2, 2, 512, 256),
            fixed(2, 512, 256),
            fixed(2, 512, 256),
            fixed(2, 2, 512, 256),
        ],
        scratch_shapes=[pltpu.VMEM((384, 512), BF16)],
    )
    return pl.pallas_call(
        gradients_kernel,
        name="gradients",
        grid_spec=spec,
        out_shape=[
            shape((512, 384)),
            shape((8, 512), F32),
            shape((2, 2, 512, 256)),
            shape((2, 2, 512, 256)),
            shape((2, 512, 256)),
            shape((2, 512, 256)),
            shape((2, 2, 512, 256)),
        ],
        compiler_params=PARAMS,
    )(idx, dkv, dq, q, kv, normed, normed, dwo, dwo)


def add_kernel(*refs):
    total = refs[0][...].astype(F32)
    for t in refs[1:-1]:
        total = total + t[...].astype(F32)
    refs[-1][...] = total.astype(BF16)


def add_blocks(terms, specs):
    return pl.pallas_call(
        add_kernel,
        name="add_blocks",
        grid=(2,),
        in_specs=specs,
        out_specs=pl.BlockSpec((None, 512, 256), lambda i: (i, 0, 0)),
        out_shape=shape((2, 512, 256)),
        compiler_params=PARAMS,
    )(*terms)


def input_grad_kernel(idx, g, g2, w, w2, dots, dots2, *outs):
    rows = split_rows(dots[0:1] + dots2[0:1])
    for n in range(8):
        out, at = outs[n // 2], idx[n]
        both = dot(g[...], w[at]) + dot(g2[...], w2[at])
        out[n % 2, 0:512, :] = both.astype(BF16)
        out[n % 2, 512:528, :] = rows


def input_grad(idx, g, g2, w, w2, dots, dots2):
    vmem = pl.BlockSpec(memory_space=pltpu.VMEM)
    return pl.pallas_call(
        input_grad_kernel,
        name="input_grad",
        in_specs=[SMEM] + [vmem] * 6,
        out_shape=[shape((2, 528, 256))] * 4,
        compiler_params=PARAMS,
    )(idx, g, g2, w, w2, dots, dots2)


def weight_grad_kernel(left, right, out):
    for k in range(right.shape[0]):
        out[k] = dot(left[...], right[k]).astype(BF16)


def weight_grad(left, right):
    rows = left.shape[0]
    return pl.pallas_call(
        weight_grad_kernel,
        name="weight_grad",
        grid=(2,),
        in_specs=[fixed(rows, 512), pl.BlockSpec((8, 512, 256), lambda j: (j, 0, 0))],
        out_specs=pl.BlockSpec((8, rows, 256), lambda j: (j, 0, 0)),
        out_shape=shape((16, rows, 256)),
        compiler_params=PARAMS,
    )(left, right)


def line_kernel(side, *refs):
    terms, (x, x_next, inv, mod, own, own_dots, sent, gains) = refs[:4], refs[4:]
    second = mod[...] == 1
    for slot, block in ((0, x), (1, x_next)):
        total = terms[0][slot, 0:512].astype(F32)
        dots = joined_rows(terms[0][slot, 512:528])
        for t in terms[1:]:
            total = total + t[slot, 0:512].astype(F32)
            dots = dots + joined_rows(t[slot, 512:528])
        if slot == 0:
            own[...] = total
            own_dots[0:2] = dots
        else:
            sent[0:512] = total.astype(BF16)
            sent[512:528] = split_rows(jnp.concatenate([dots[0:1], dots[1:2]], axis=1))
        each = total * (block[...].astype(F32) * inv[...])
        first = jnp.sum(jnp.where(second, 0.0, each), axis=0, keepdims=True)
        other = jnp.sum(jnp.where(second, each, 0.0), axis=0, keepdims=True)
        at = side[0] if slot == 0 else 1 - side[0]
        for k in range(8):
            gains[k, at, 0:1] = first
            gains[k, at, 1:2] = other


def line_sum(side, terms, x, x_next, inv, modality):
    return pl.pallas_call(
        line_kernel,
        name="line_sum",
        grid=(1,),
        in_specs=[SMEM]
        + [fixed(2, 528, 256)] * 4
        + [fixed(512, 256), fixed(512, 256), fixed(512, 1), fixed(512, 1)],
        out_specs=[fixed(512, 256), fixed(8, 256), fixed(528, 256), fixed(8, 2, 2, 256)],
        out_shape=[
            shape((512, 256), F32),
            shape((8, 256), F32),
            shape((528, 256)),
            shape((8, 2, 2, 256), F32),
        ],
        compiler_params=PARAMS,
    )(side, *terms, x, x_next, inv, modality)


def finish_kernel(own, own_dots, last, x, inv, mod, gain, grad_in):
    gn = own[...] + last[0:512].astype(F32)
    dots = own_dots[0:2] + joined_rows(last[512:528])
    columns = [jnp.broadcast_to(dots[r : r + 1], (128, 256)).T[:, 0:1] for r in range(2)]
    mean = jnp.concatenate(columns, axis=0) / 4096
    scaled = x[...].astype(F32) * inv[...]
    up = gn * jnp.where(mod[...] == 1, gain[1:2], gain[0:1])
    grad_in[...] = (inv[...] * (up - scaled * mean)).astype(BF16)


def finish(own, own_dots, last, x, inv, modality, gain):
    return pl.pallas_call(
        finish_kernel,
        name="finish",
        out_shape=shape((512, 256)),
        compiler_params=PARAMS,
    )(own, own_dots, last, x, inv, modality, gain)


def output_kernel(idx, *refs):
    atts, (rows, out) = refs[:16], refs[16:]
    total = jnp.zeros(out.shape, F32)
    for n in range(16):
        total = total + dot(atts[n][...], rows[idx[n]]).astype(BF16).astype(F32)
    out[...] = total.astype(BF16)


def output(idx, atts, rows):
    tile = 128
    return pl.pallas_call(
        output_kernel,
        name="output",
        grid=(512 // tile,),
        in_specs=[SMEM]
        + [pl.BlockSpec((tile, 128), lambda i: (i, 0))] * 16
        + [fixed(16, 128, 256)],
        out_specs=pl.BlockSpec((tile, 256), lambda i: (i, 0)),
        out_shape=shape((512, 256)),
        compiler_params=PARAMS,
    )(idx, *atts, rows)


def sum_weights_kernel(*refs):
    parts, (qkv, wout) = refs[:5], refs[5:]
    total = parts[0][...].astype(F32)
    for t in parts[1:]:
        total = total + t[...].astype(F32)
    for m in range(3):
        qkv[m] = total[m * 128 : (m + 1) * 128].T
    wout[...] = total[384:512]


ONE = pl.BlockSpec((None, 512, 256), lambda i: (i, 0, 0))
FIRST = pl.BlockSpec((None, None, 512, 256), lambda i: (0, i, 0, 0))
SECOND = pl.BlockSpec((None, None, 512, 256), lambda i: (1, i, 0, 0))


def sum_weights(parts):
    return pl.pallas_call(
        sum_weights_kernel,
        name="sum_weights",
        grid=(2,),
        in_specs=[FIRST, FIRST, FIRST, ONE, ONE],
        out_specs=[
            pl.BlockSpec((3, 256, 128), lambda s: (0, s, 0)),
            pl.BlockSpec((128, 256), lambda s: (0, s)),
        ],
        out_shape=[shape((3, 512, 128), F32), shape((128, 512), F32)],
        compiler_params=PARAMS,
    )(*parts)


def sublayer(layer_input, modality, image_spans, norm_gain, w_qkv, w_out, grad_out):
    x, h, c = (lax.axis_index(a) for a in GROUP)
    z, u = (lax.axis_index(a) for a in TOKENS_AXES)
    blocks = [((x - d) % 4, h ^ s, c ^ k) for k in range(2) for s in range(2) for d in TURNS]
    idx = jnp.stack([a * 4 + b * 2 + e for a, b, e in blocks]).astype(jnp.int32)
    tok_idx = jnp.stack([((z - d) % 4) * 2 + (u ^ s) for s in range(2) for d in TURNS]).astype(jnp.int32)
    places = jnp.stack([((x + d) % 4) * 2 + (h ^ s) for d in range(4) for s in range(2)]).astype(jnp.int32)
    outward = [((z + d) % 4) * 2 + (u ^ s) for d in (1, 3, 2, 0) for s in range(2)]
    out_idx = jnp.stack(outward).astype(jnp.int32)
    core = c.astype(jnp.int32)[None]
    side = h.astype(jnp.int32)[None]
    column = modality[:, None]

    gain_rows = jnp.concatenate(three_parts(norm_gain), axis=0).astype(BF16)
    gain_rows = jnp.concatenate([gain_rows, jnp.zeros((10, 256), BF16)], axis=0)
    xs = spread(jnp.concatenate([layer_input, gain_rows], axis=0))
    ws = gather_tokens_axes(pack_weights(w_qkv, w_out))
    gs = spread(grad_out)

    normed, inv = normalize(idx, xs, column)
    q, kv = project(tok_idx, normed, ws)
    kvs = gather_tokens_axes(kv)
    w_kept, w_sent = order_weights(tok_idx, core, ws)
    w_other = swap(w_sent, "c")
    da, g_all, wo = upstream(idx, tok_idx, gs, ws)

    pos = (z * 2 + u) * 512 + jnp.arange(512, dtype=jnp.int32)
    inside = (pos[:, None] >= image_spans[0][None]) & (pos[:, None] < image_spans[1][None])
    ends = jnp.max(jnp.where(inside, image_spans[1][None], 0), axis=1)
    limit = jnp.maximum(pos + 1, ends)[None, :]

    out_rows = exchange(wo, GROUP)
    att, att_t, lse, all_kv = forward(tok_idx, limit, q, kvs)
    dq, dkv = backward(limit, lse, q, all_kv, da, att_t)
    dkv_parts = exchange(dkv.reshape(8, 512, 256), TOKENS_AXES)

    dwo = weight_grad(att_t, g_all)
    atts = spread(att)
    attn_out = output(idx, atts, out_rows)

    g, dots, up, down, far, far_next, here = gradients(out_idx, dkv_parts, dq, q, kv, normed, dwo)
    far_next = swap(far_next, "u")
    up, down = turn(up, 1, "z"), turn(down, 3, "z")
    far = turn(add_blocks([far, far_next], [ONE, ONE]), 2, "z")
    across = swap(add_blocks([here, up, down], [SECOND] * 3), "u")
    g2, dots2 = swap(g, "c"), swap(dots, "c")
    terms = input_grad(places, g, g2, w_kept, w_other, dots, dots2)
    terms = [turn(t, d) if d else t for d, t in enumerate(terms)]
    own, own_dots, sent, gains = line_sum(side, terms, layer_input, xs[4], inv, column)
    last = swap(sent, "h")
    gains = exchange(gains.reshape(16, 2, 256), ("z", "u", "h"))
    grad_in = finish(own, own_dots, last, layer_input, inv, column, norm_gain)
    grad_qkv, grad_wout = sum_weights([here, up, down, far, across])
    grad_gain = jnp.sum(gains, axis=0)
    return (attn_out, grad_in, grad_qkv, grad_wout, grad_gain)


def solution(mesh):
    fine = Mesh(mesh.devices.reshape(4, 2, 2, 4, 2), ("x", "h", "c", "z", "u"))
    tok, feat = TOKENS_AXES, GROUP
    in_specs = (P(tok, feat), P(tok), P(), P(None, feat), P(None, tok, feat), P(feat, tok), P(tok, feat))
    out_specs = (P(tok, feat), P(tok, feat), P(None, tok, feat), P(feat, tok), P(None, feat))
    return jax.shard_map(sublayer, mesh=fine, in_specs=in_specs, out_specs=out_specs, check_vma=False)
```

```python
import math

import jax
import jax.numpy as jnp
from jax import lax
from jax.experimental import pallas as pl
from jax.experimental.pallas import tpu as pltpu
from jax.sharding import Mesh
from jax.sharding import PartitionSpec as P


epsilon = 1e-05
masked_low = -1e30
GROUP = ("x", "h", "c")
TOKENS_AXES = ("z", "u")
F32 = jnp.float32
BF16 = jnp.bfloat16
TURNS = (0, 1, 3, 2)
NT = (((1,), (1,)), ((), ()))
TN = (((0,), (0,)), ((), ()))
SMEM = pl.BlockSpec(memory_space=pltpu.SMEM)
PARAMS = pltpu.CompilerParams(vmem_limit_bytes=60 * 1024 * 1024)


def swap(a, axis):
    return lax.ppermute(a, axis, [(0, 1), (1, 0)])


def turn(a, d, axis="x"):
    return lax.ppermute(a, axis, [(i, (i + d) % 4) for i in range(4)])


def turns(a, axis="x"):
    return [a] + [turn(a, d, axis) for d in TURNS[1:]]


def spread(block):
    other = swap(block, "h")
    pair = jnp.stack([block, other])
    row = turns(pair)
    return row + [swap(a, "c") for a in row]


def gather_tokens_axes(block):
    own = [block] + [turn(block, d, "z") for d in (1, 3)]
    own.append(turn(block, 2, "z"))
    near = swap(block, "u")
    near = [near] + [turn(near, d, "z") for d in (1, 3)]
    return own + near + [swap(own[3], "u")]


def exchange(blocks, axis):
    return lax.all_to_all(blocks, axis, 0, 0, tiled=True)


def three_parts(g):
    high = lax.reduce_precision(g, 8, 7)
    rest = g - high
    mid = lax.reduce_precision(rest, 8, 7)
    return high, mid, rest - mid


def dot(a, b, dims=(((1,), (0,)), ((), ()))):
    return lax.dot_general(a, b, dims, preferred_element_type=F32)


def shape(dims, kind=BF16):
    return jax.ShapeDtypeStruct(dims, kind)


def fixed(*dims):
    return pl.BlockSpec(dims, lambda *i: (0,) * len(dims))


def pack_kernel(w, wo, out):
    for s in range(2):
        for m in range(3):
            out[s, m * 128 : (m + 1) * 128, :] = w[m, s * 256 : (s + 1) * 256, :].T
        out[s, 384:512, :] = wo[:, s * 256 : (s + 1) * 256]


def pack_weights(w, wo):
    return pl.pallas_call(
        pack_kernel,
        name="pack_weights",
        out_shape=shape((2, 512, 256)),
        compiler_params=PARAMS,
    )(w, wo)


def normalize_kernel(idx, *refs):
    xs, gains = refs[:8], refs[8:16]
    mod, normed, inv_out = refs[16:]
    rows = mod.shape[0]
    squares = jnp.zeros((rows, 256), F32)
    for a in xs:
        for s in range(2):
            xb = a[s].astype(F32)
            squares = squares + xb * xb
    inv = lax.rsqrt(jnp.sum(squares, axis=1, keepdims=True) / 4096 + epsilon)
    inv_out[...] = inv
    second = mod[...] == 1
    for n in range(16):
        g = gains[n // 2][n % 2].astype(F32)
        g0 = (g[0:1] + g[2:3]) + g[4:5]
        g1 = (g[1:2] + g[3:4]) + g[5:6]
        scaled = xs[n // 2][n % 2].astype(F32) * inv
        normed[idx[n]] = (scaled * jnp.where(second, g1, g0)).astype(BF16)


def normalize(idx, xs, modality):
    tile = 128
    rows = lambda cols: pl.BlockSpec((tile, cols), lambda i: (i, 0))
    return pl.pallas_call(
        normalize_kernel,
        name="normalize",
        grid=(512 // tile,),
        in_specs=[SMEM]
        + [pl.BlockSpec((2, tile, 256), lambda i: (0, i, 0))] * 8
        + [pl.BlockSpec((2, 16, 256), lambda i: (0, 32, 0))] * 8
        + [rows(1)],
        out_specs=[pl.BlockSpec((16, tile, 256), lambda i: (0, i, 0)), rows(1)],
        out_shape=[shape((16, 512, 256)), shape((512, 1), F32)],
        compiler_params=PARAMS,
    )(idx, *xs, *xs, modality)


def project_kernel(idx, normed, *refs):
    ws, (q, kv) = refs[:8], refs[8:]
    total = jnp.zeros((q.shape[0], 384), F32)
    for n in range(8):
        for s in range(2):
            total = total + dot(normed[idx[n] * 2 + s], ws[n][s], NT)
    both = total.astype(BF16)
    q[...] = both[:, 0:128]
    kv[...] = both[:, 128:384]


def project(idx, normed, ws):
    tile = 256
    rows = lambda cols: pl.BlockSpec((tile, cols), lambda i: (i, 0))
    return pl.pallas_call(
        project_kernel,
        name="project",
        grid=(512 // tile,),
        in_specs=[SMEM, pl.BlockSpec((16, tile, 256), lambda i: (0, i, 0))] + [fixed(2, 384, 256)] * 8,
        out_specs=[rows(128), rows(256)],
        out_shape=[shape((512, 128)), shape((512, 256))],
        compiler_params=PARAMS,
    )(idx, normed, *ws)


def order_kernel(idx, core, *refs):
    ws, (kept, sent) = refs[:8], refs[8:]
    for n in range(8):
        k = idx[n]
        kept[k] = ws[n][core[0]]
        sent[k] = ws[n][1 - core[0]]


def order_weights(idx, core, ws):
    return pl.pallas_call(
        order_kernel,
        name="order_weights",
        grid=(1,),
        in_specs=[SMEM, SMEM] + [fixed(2, 384, 256)] * 8,
        out_specs=[fixed(8, 384, 256)] * 2,
        out_shape=[shape((8, 384, 256))] * 2,
        compiler_params=PARAMS,
    )(idx, core, *ws)


def upstream_kernel(idx, tok_idx, *refs):
    gs, ws, (out, ordered, wo) = refs[:8], refs[8:16], refs[16:]

    @pl.when(pl.program_id(0) == 0)
    def _():
        for n in range(8):
            for s in range(2):
                wo[tok_idx[n] * 2 + s] = ws[n][s]

    acc = jnp.zeros(out.shape, F32)
    for n in range(16):
        g = gs[n // 2][n % 2]
        ordered[idx[n]] = g
        acc = acc + dot(g, wo[idx[n]], NT)
    out[...] = acc.astype(BF16)


def upstream(idx, tok_idx, gs, ws):
    tile = 128
    return pl.pallas_call(
        upstream_kernel,
        name="upstream",
        grid=(512 // tile,),
        in_specs=[SMEM, SMEM]
        + [pl.BlockSpec((2, tile, 256), lambda i: (0, i, 0))] * 8
        + [pl.BlockSpec((2, 128, 256), lambda i: (0, 3, 0))] * 8,
        out_specs=[
            pl.BlockSpec((tile, 128), lambda i: (i, 0)),
            pl.BlockSpec((16, tile, 256), lambda i: (0, i, 0)),
            fixed(16, 128, 256),
        ],
        out_shape=[shape((512, 128)), shape((16, 512, 256)), shape((16, 128, 256))],
        compiler_params=PARAMS,
    )(idx, tok_idx, *gs, *ws)


KEY_BLOCK = 512
SCALE = 1.0 / math.sqrt(128)
TO_BASE2 = SCALE * math.log2(math.e)


def masked_scores(b, kv, q, edge):
    s = dot(kv[pl.ds(b * KEY_BLOCK, KEY_BLOCK), 0:128], q[...], NT) * TO_BASE2
    pos = lax.broadcasted_iota(jnp.int32, s.shape, 0) + b * KEY_BLOCK
    return jnp.where(pos < edge, s, masked_low)


def forward_kernel(idx, limit, q, *refs):
    parts, (att, att_t, lse, kv, s_all) = refs[:8], refs[8:]
    for n in range(8):
        kv[pl.ds(idx[n] * 512, 512), :] = parts[n][...]
    count = kv.shape[0] // KEY_BLOCK
    cols = q.shape[0]
    edge = limit[...]

    def scores(b, top):
        s = masked_scores(b, kv, q, edge)
        s_all[pl.ds(b * KEY_BLOCK, KEY_BLOCK), :] = s
        return jnp.maximum(top, jnp.max(s, axis=0, keepdims=True))

    top = lax.fori_loop(0, count, scores, jnp.full((1, cols), masked_low, F32))

    def sums(b, total):
        at = pl.ds(b * KEY_BLOCK, KEY_BLOCK)
        e = jnp.exp2(s_all[at, :] - top)
        s_all[at, :] = e
        return total + jnp.sum(e, axis=0, keepdims=True)

    total = lax.fori_loop(0, count, sums, jnp.zeros((1, cols), F32))
    inv = 1.0 / total
    lse[...] = top + jnp.log2(total)

    def attend(b, acc):
        at = pl.ds(b * KEY_BLOCK, KEY_BLOCK)
        return acc + dot(kv[at, 128:256], (s_all[at, :] * inv).astype(BF16), TN)

    out_t = lax.fori_loop(0, count, attend, jnp.zeros((128, cols), F32)).astype(BF16)
    att_t[...] = out_t
    att[...] = out_t.T


def forward(idx, limit, q, parts):
    vmem = pl.BlockSpec(memory_space=pltpu.VMEM)
    return pl.pallas_call(
        forward_kernel,
        name="forward",
        in_specs=[SMEM] + [vmem] * 10,
        out_shape=[shape((512, 128)), shape((128, 512)), shape((1, 512), F32), shape((4096, 256))],
        scratch_shapes=[pltpu.VMEM((4096, 512), F32)],
        compiler_params=PARAMS,
    )(idx, limit, q, *parts)


def backward_kernel(limit, lse, q, kv, da, att_t, dq, dkv):
    count = kv.shape[0] // KEY_BLOCK
    edge = limit[...]
    da_t = da[...].T
    row_dots = jnp.sum(att_t[...].astype(F32) * da_t.astype(F32), axis=0, keepdims=True)

    def back(b, acc):
        at = pl.ds(b * KEY_BLOCK, KEY_BLOCK)
        p = jnp.exp2(masked_scores(b, kv, q, edge) - lse[...])
        d_probs = dot(kv[at, 128:256], da[...], NT)
        ds = (p * (d_probs - row_dots) * SCALE).astype(BF16)
        dkv[at, 0:128] = dot(ds, q[...]).astype(BF16)
        dkv[at, 128:256] = dot(p.astype(BF16), da[...]).astype(BF16)
        return acc + dot(kv[at, 0:128], ds, TN)

    dq_t = lax.fori_loop(0, count, back, jnp.zeros((128, q.shape[0]), F32))
    dq[...] = dq_t.astype(BF16).T


def backward(limit, lse, q, kv, da, att_t):
    return pl.pallas_call(
        backward_kernel,
        name="backward",
        out_shape=[shape((512, 128)), shape((4096, 256))],
        compiler_params=PARAMS,
    )(limit, lse, q, kv, da, att_t)


def split_rows(dots):
    rows = []
    for p in (dots[:, 0:256], dots[:, 256:512]):
        high = p.astype(BF16).astype(F32)
        mid = (p - high).astype(BF16).astype(F32)
        rows.append((high, mid, p - high - mid))
    kind = lax.broadcasted_iota(jnp.int32, (16, 256), 0)
    both = jnp.zeros((16, 256), F32)
    for r in range(6):
        both = jnp.where(kind == r, rows[r % 2][r // 2], both)
    return both.astype(BF16)


def joined_rows(block):
    t = block.astype(F32)
    return (t[0:2] + t[2:4]) + t[4:6]


def gradients_kernel(idx, dkv, dq, q, kv, n0, n1, w0, w1, g_out, dots, up, down, far, far_next, here, g_t):
    step = pl.program_id(0)

    @pl.when(step == 0)
    def _():
        total = dkv[0].astype(F32)
        for k in range(1, 8):
            total = total + dkv[k].astype(F32)
        g = jnp.concatenate([dq[...], total.astype(BF16)], axis=1)
        g_out[...] = g
        g_t[...] = g.T
        gf = g.astype(F32)
        prod = gf[:, 0:128] * q[...].astype(F32)
        prod = prod + gf[:, 128:256] * kv[:, 0:128].astype(F32)
        prod = prod + gf[:, 256:384] * kv[:, 128:256].astype(F32)
        ones = jnp.ones((8, 128), F32)
        dots[...] = lax.dot_general(
            ones, prod, NT, precision=lax.Precision.HIGHEST, preferred_element_type=F32
        )

    outs = ((up.at[0], up.at[1]), (down.at[0], down.at[1]), (far, far_next), (here.at[0], here.at[1]))
    for n, pair in enumerate(outs):

        @pl.when(step == n + 1)
        def _(pair=pair):
            for out, block, wo in ((pair[0], n0, w0), (pair[1], n1, w1)):
                for k in range(2):
                    out[k, 0:384, :] = dot(g_t[...], block[k]).astype(BF16)
                    out[k, 384:512, :] = wo[k]


def gradients(idx, dkv, dq, q, kv, normed, dwo):
    at = lambda slot: lambda i, idx: (idx[2 * jnp.maximum(i - 1, 0) + slot], 0, 0)
    spec = pltpu.PrefetchScalarGridSpec(
        num_scalar_prefetch=1,
        grid=(5,),
        in_specs=[
            fixed(8, 512, 256),
            fixed(512, 128),
            fixed(512, 128),
            fixed(512, 256),
            pl.BlockSpec((2, 512, 256), at(0)),
            pl.BlockSpec((2, 512, 256), at(1)),
            pl.BlockSpec((2, 128, 256), at(0)),
            pl.BlockSpec((2, 128, 256), at(1)),
        ],
        out_specs=[
            fixed(512, 384),
            fixed(8, 512),
            fixed(2, 2, 512, 256),
            fixed(2, 2, 512, 256),
            fixed(2, 512, 256),
            fixed(2, 512, 256),
            fixed(2, 2, 512, 256),
        ],
        scratch_shapes=[pltpu.VMEM((384, 512), BF16)],
    )
    return pl.pallas_call(
        gradients_kernel,
        name="gradients",
        grid_spec=spec,
        out_shape=[
            shape((512, 384)),
            shape((8, 512), F32),
            shape((2, 2, 512, 256)),
            shape((2, 2, 512, 256)),
            shape((2, 512, 256)),
            shape((2, 512, 256)),
            shape((2, 2, 512, 256)),
        ],
        compiler_params=PARAMS,
    )(idx, dkv, dq, q, kv, normed, normed, dwo, dwo)


def add_kernel(*refs):
    total = refs[0][...].astype(F32)
    for t in refs[1:-1]:
        total = total + t[...].astype(F32)
    refs[-1][...] = total.astype(BF16)


def add_blocks(terms, specs):
    return pl.pallas_call(
        add_kernel,
        name="add_blocks",
        grid=(2,),
        in_specs=specs,
        out_specs=pl.BlockSpec((None, 512, 256), lambda i: (i, 0, 0)),
        out_shape=shape((2, 512, 256)),
        compiler_params=PARAMS,
    )(*terms)


def input_grad_kernel(idx, g, g2, w, w2, dots, dots2, *outs):
    rows = split_rows(dots[0:1] + dots2[0:1])
    for n in range(8):
        out, at = outs[n // 2], idx[n]
        both = dot(g[...], w[at]) + dot(g2[...], w2[at])
        out[n % 2, 0:512, :] = both.astype(BF16)
        out[n % 2, 512:528, :] = rows


def input_grad(idx, g, g2, w, w2, dots, dots2):
    vmem = pl.BlockSpec(memory_space=pltpu.VMEM)
    return pl.pallas_call(
        input_grad_kernel,
        name="input_grad",
        in_specs=[SMEM] + [vmem] * 6,
        out_shape=[shape((2, 528, 256))] * 4,
        compiler_params=PARAMS,
    )(idx, g, g2, w, w2, dots, dots2)


def weight_grad_kernel(left, right, out):
    for k in range(right.shape[0]):
        out[k] = dot(left[...], right[k]).astype(BF16)


def weight_grad(left, right):
    rows = left.shape[0]
    return pl.pallas_call(
        weight_grad_kernel,
        name="weight_grad",
        grid=(2,),
        in_specs=[fixed(rows, 512), pl.BlockSpec((8, 512, 256), lambda j: (j, 0, 0))],
        out_specs=pl.BlockSpec((8, rows, 256), lambda j: (j, 0, 0)),
        out_shape=shape((16, rows, 256)),
        compiler_params=PARAMS,
    )(left, right)


def line_kernel(side, *refs):
    terms, (x, x_next, inv, mod, own, own_dots, sent, gains) = refs[:4], refs[4:]
    second = mod[...] == 1
    for slot, block in ((0, x), (1, x_next)):
        total = terms[0][slot, 0:512].astype(F32)
        dots = joined_rows(terms[0][slot, 512:528])
        for t in terms[1:]:
            total = total + t[slot, 0:512].astype(F32)
            dots = dots + joined_rows(t[slot, 512:528])
        if slot == 0:
            own[...] = total
            own_dots[0:2] = dots
        else:
            sent[0:512] = total.astype(BF16)
            sent[512:528] = split_rows(jnp.concatenate([dots[0:1], dots[1:2]], axis=1))
        each = total * (block[...].astype(F32) * inv[...])
        first = jnp.sum(jnp.where(second, 0.0, each), axis=0, keepdims=True)
        other = jnp.sum(jnp.where(second, each, 0.0), axis=0, keepdims=True)
        at = side[0] if slot == 0 else 1 - side[0]
        for k in range(8):
            gains[k, at, 0:1] = first
            gains[k, at, 1:2] = other


NEXT = pl.BlockSpec((None, 512, 256), lambda i: (1, 0, 0))


def line_sum(side, terms, x, x_next, inv, modality):
    return pl.pallas_call(
        line_kernel,
        name="line_sum",
        grid=(1,),
        in_specs=[SMEM]
        + [fixed(2, 528, 256)] * 4
        + [fixed(512, 256), NEXT, fixed(512, 1), fixed(512, 1)],
        out_specs=[fixed(512, 256), fixed(8, 256), fixed(528, 256), fixed(8, 2, 2, 256)],
        out_shape=[
            shape((512, 256), F32),
            shape((8, 256), F32),
            shape((528, 256)),
            shape((8, 2, 2, 256), F32),
        ],
        compiler_params=PARAMS,
    )(side, *terms, x, x_next, inv, modality)


def finish_kernel(own, own_dots, last, x, inv, mod, gain, grad_in):
    gn = own[...] + last[0:512].astype(F32)
    dots = own_dots[0:2] + joined_rows(last[512:528])
    columns = [jnp.broadcast_to(dots[r : r + 1], (128, 256)).T[:, 0:1] for r in range(2)]
    mean = jnp.concatenate(columns, axis=0) / 4096
    scaled = x[...].astype(F32) * inv[...]
    up = gn * jnp.where(mod[...] == 1, gain[1:2], gain[0:1])
    grad_in[...] = (inv[...] * (up - scaled * mean)).astype(BF16)


def finish(own, own_dots, last, x, inv, modality, gain):
    return pl.pallas_call(
        finish_kernel,
        name="finish",
        out_shape=shape((512, 256)),
        compiler_params=PARAMS,
    )(own, own_dots, last, x, inv, modality, gain)


def output_kernel(idx, *refs):
    atts, (rows, out) = refs[:8], refs[8:]
    total = jnp.zeros(out.shape, F32)
    for n in range(16):
        total = total + dot(atts[n // 2][n % 2], rows[idx[n]]).astype(BF16).astype(F32)
    out[...] = total.astype(BF16)


def output(idx, atts, rows):
    tile = 128
    return pl.pallas_call(
        output_kernel,
        name="output",
        grid=(512 // tile,),
        in_specs=[SMEM]
        + [pl.BlockSpec((2, tile, 128), lambda i: (0, i, 0))] * 8
        + [fixed(16, 128, 256)],
        out_specs=pl.BlockSpec((tile, 256), lambda i: (i, 0)),
        out_shape=shape((512, 256)),
        compiler_params=PARAMS,
    )(idx, *atts, rows)


def sum_weights_kernel(*refs):
    parts, (qkv, wout) = refs[:5], refs[5:]
    total = parts[0][...].astype(F32)
    for t in parts[1:]:
        total = total + t[...].astype(F32)
    for m in range(3):
        qkv[m] = total[m * 128 : (m + 1) * 128].T
    wout[...] = total[384:512]


ONE = pl.BlockSpec((None, 512, 256), lambda i: (i, 0, 0))
FIRST = pl.BlockSpec((None, None, 512, 256), lambda i: (0, i, 0, 0))
SECOND = pl.BlockSpec((None, None, 512, 256), lambda i: (1, i, 0, 0))


def sum_weights(parts):
    return pl.pallas_call(
        sum_weights_kernel,
        name="sum_weights",
        grid=(2,),
        in_specs=[FIRST, FIRST, FIRST, ONE, ONE],
        out_specs=[
            pl.BlockSpec((3, 256, 128), lambda s: (0, s, 0)),
            pl.BlockSpec((128, 256), lambda s: (0, s)),
        ],
        out_shape=[shape((3, 512, 128), F32), shape((128, 512), F32)],
        compiler_params=PARAMS,
    )(*parts)


def sublayer(layer_input, modality, image_spans, norm_gain, w_qkv, w_out, grad_out):
    x, h, c = (lax.axis_index(a) for a in GROUP)
    z, u = (lax.axis_index(a) for a in TOKENS_AXES)
    blocks = [((x - d) % 4, h ^ s, c ^ k) for k in range(2) for d in TURNS for s in range(2)]
    idx = jnp.stack([a * 4 + b * 2 + e for a, b, e in blocks]).astype(jnp.int32)
    tok_idx = jnp.stack([((z - d) % 4) * 2 + (u ^ s) for s in range(2) for d in TURNS]).astype(jnp.int32)
    places = jnp.stack([((x + d) % 4) * 2 + (h ^ s) for d in range(4) for s in range(2)]).astype(jnp.int32)
    outward = [((z + d) % 4) * 2 + (u ^ s) for d in (1, 3, 2, 0) for s in range(2)]
    out_idx = jnp.stack(outward).astype(jnp.int32)
    core = c.astype(jnp.int32)[None]
    side = h.astype(jnp.int32)[None]
    column = modality[:, None]

    gain_rows = jnp.concatenate(three_parts(norm_gain), axis=0).astype(BF16)
    gain_rows = jnp.concatenate([gain_rows, jnp.zeros((10, 256), BF16)], axis=0)
    xs = spread(jnp.concatenate([layer_input, gain_rows], axis=0))
    ws = gather_tokens_axes(pack_weights(w_qkv, w_out))
    gs = spread(grad_out)

    normed, inv = normalize(idx, xs, column)
    q, kv = project(tok_idx, normed, ws)
    kvs = gather_tokens_axes(kv)
    w_kept, w_sent = order_weights(tok_idx, core, ws)
    w_other = swap(w_sent, "c")
    da, g_all, wo = upstream(idx, tok_idx, gs, ws)

    pos = (z * 2 + u) * 512 + jnp.arange(512, dtype=jnp.int32)
    inside = (pos[:, None] >= image_spans[0][None]) & (pos[:, None] < image_spans[1][None])
    ends = jnp.max(jnp.where(inside, image_spans[1][None], 0), axis=1)
    limit = jnp.maximum(pos + 1, ends)[None, :]

    out_rows = exchange(wo, GROUP)
    att, att_t, lse, all_kv = forward(tok_idx, limit, q, kvs)
    dq, dkv = backward(limit, lse, q, all_kv, da, att_t)
    dkv_parts = exchange(dkv.reshape(8, 512, 256), TOKENS_AXES)

    dwo = weight_grad(att_t, g_all)
    atts = spread(att)
    attn_out = output(idx, atts, out_rows)

    g, dots, up, down, far, far_next, here = gradients(out_idx, dkv_parts, dq, q, kv, normed, dwo)
    far_next = swap(far_next, "u")
    up, down = turn(up, 1, "z"), turn(down, 3, "z")
    far = turn(add_blocks([far, far_next], [ONE, ONE]), 2, "z")
    across = swap(add_blocks([here, up, down], [SECOND] * 3), "u")
    g2, dots2 = swap(g, "c"), swap(dots, "c")
    terms = input_grad(places, g, g2, w_kept, w_other, dots, dots2)
    terms = [turn(t, d) if d else t for d, t in enumerate(terms)]
    own, own_dots, sent, gains = line_sum(side, terms, layer_input, xs[0], inv, column)
    last = swap(sent, "h")
    gains = exchange(gains.reshape(16, 2, 256), ("z", "u", "h"))
    grad_in = finish(own, own_dots, last, layer_input, inv, column, norm_gain)
    grad_qkv, grad_wout = sum_weights([here, up, down, far, across])
    grad_gain = jnp.sum(gains, axis=0)
    return (attn_out, grad_in, grad_qkv, grad_wout, grad_gain)


def solution(mesh):
    fine = Mesh(mesh.devices.reshape(4, 2, 2, 4, 2), ("x", "h", "c", "z", "u"))
    tok, feat = TOKENS_AXES, GROUP
    in_specs = (P(tok, feat), P(tok), P(), P(None, feat), P(None, tok, feat), P(feat, tok), P(tok, feat))
    out_specs = (P(tok, feat), P(tok, feat), P(None, tok, feat), P(feat, tok), P(None, feat))
    return jax.shard_map(sublayer, mesh=fine, in_specs=in_specs, out_specs=out_specs, check_vma=False)
```

```python
import math

import jax
import jax.numpy as jnp
from jax import lax
from jax.experimental import pallas as pl
from jax.experimental.pallas import tpu as pltpu
from jax.sharding import Mesh
from jax.sharding import PartitionSpec as P


epsilon = 1e-05
masked_low = -1e30
GROUP = ("x", "h", "c")
TOKENS_AXES = ("z", "u")
F32 = jnp.float32
BF16 = jnp.bfloat16
TURNS = (0, 1, 3, 2)
NT = (((1,), (1,)), ((), ()))
TN = (((0,), (0,)), ((), ()))
SMEM = pl.BlockSpec(memory_space=pltpu.SMEM)
PARAMS = pltpu.CompilerParams(vmem_limit_bytes=60 * 1024 * 1024)


def swap(a, axis):
    return lax.ppermute(a, axis, [(0, 1), (1, 0)])


def turn(a, d, axis="x"):
    return lax.ppermute(a, axis, [(i, (i + d) % 4) for i in range(4)])


def turns(a, axis="x"):
    return [a] + [turn(a, d, axis) for d in TURNS[1:]]


def spread(block):
    other = swap(block, "h")
    pair = jnp.stack([block, other])
    row = turns(pair)
    return row + [swap(a, "c") for a in row]


def gather_tokens_axes(block):
    own = [block] + [turn(block, d, "z") for d in (1, 3)]
    own.append(turn(block, 2, "z"))
    near = swap(block, "u")
    near = [near] + [turn(near, d, "z") for d in (1, 3)]
    return own + near + [swap(own[3], "u")]


def exchange(blocks, axis):
    return lax.all_to_all(blocks, axis, 0, 0, tiled=True)


def three_parts(g):
    high = lax.reduce_precision(g, 8, 7)
    rest = g - high
    mid = lax.reduce_precision(rest, 8, 7)
    return high, mid, rest - mid


def dot(a, b, dims=(((1,), (0,)), ((), ()))):
    return lax.dot_general(a, b, dims, preferred_element_type=F32)


def shape(dims, kind=BF16):
    return jax.ShapeDtypeStruct(dims, kind)


def fixed(*dims):
    return pl.BlockSpec(dims, lambda *i: (0,) * len(dims))


def pack_kernel(w, wo, out):
    for s in range(2):
        for m in range(3):
            out[s, m * 128 : (m + 1) * 128, :] = w[m, s * 256 : (s + 1) * 256, :].T
        out[s, 384:512, :] = wo[:, s * 256 : (s + 1) * 256]


def pack_weights(w, wo):
    return pl.pallas_call(
        pack_kernel,
        name="pack_weights",
        out_shape=shape((2, 512, 256)),
        compiler_params=PARAMS,
    )(w, wo)


def normalize_kernel(idx, *refs):
    xs, gains = refs[:8], refs[8:16]
    mod, normed, inv_out = refs[16:]
    rows = mod.shape[0]
    squares = jnp.zeros((rows, 256), F32)
    for a in xs:
        for s in range(2):
            xb = a[s].astype(F32)
            squares = squares + xb * xb
    inv = lax.rsqrt(jnp.sum(squares, axis=1, keepdims=True) / 4096 + epsilon)
    inv_out[...] = inv
    second = mod[...] == 1
    for n in range(16):
        g = gains[n // 2][n % 2].astype(F32)
        g0 = (g[0:1] + g[2:3]) + g[4:5]
        g1 = (g[1:2] + g[3:4]) + g[5:6]
        scaled = xs[n // 2][n % 2].astype(F32) * inv
        normed[idx[n]] = (scaled * jnp.where(second, g1, g0)).astype(BF16)


def normalize(idx, xs, modality):
    tile = 256
    rows = lambda cols: pl.BlockSpec((tile, cols), lambda i: (i, 0))
    return pl.pallas_call(
        normalize_kernel,
        name="normalize",
        grid=(512 // tile,),
        in_specs=[SMEM]
        + [pl.BlockSpec((2, tile, 256), lambda i: (0, i, 0))] * 8
        + [pl.BlockSpec((2, 16, 256), lambda i: (0, 32, 0))] * 8
        + [rows(1)],
        out_specs=[pl.BlockSpec((16, tile, 256), lambda i: (0, i, 0)), rows(1)],
        out_shape=[shape((16, 512, 256)), shape((512, 1), F32)],
        compiler_params=PARAMS,
    )(idx, *xs, *xs, modality)


def project_kernel(idx, normed, *refs):
    ws, (q, kv) = refs[:8], refs[8:]
    total = jnp.zeros((q.shape[0], 384), F32)
    for n in range(8):
        for s in range(2):
            total = total + dot(normed[idx[n] * 2 + s], ws[n][s], NT)
    both = total.astype(BF16)
    q[...] = both[:, 0:128]
    kv[...] = both[:, 128:384]


def project(idx, normed, ws):
    tile = 256
    rows = lambda cols: pl.BlockSpec((tile, cols), lambda i: (i, 0))
    return pl.pallas_call(
        project_kernel,
        name="project",
        grid=(512 // tile,),
        in_specs=[SMEM, pl.BlockSpec((16, tile, 256), lambda i: (0, i, 0))] + [fixed(2, 384, 256)] * 8,
        out_specs=[rows(128), rows(256)],
        out_shape=[shape((512, 128)), shape((512, 256))],
        compiler_params=PARAMS,
    )(idx, normed, *ws)


def order_kernel(idx, core, *refs):
    ws, (kept, sent) = refs[:8], refs[8:]
    for n in range(8):
        k = idx[n]
        kept[k] = ws[n][core[0]]
        sent[k] = ws[n][1 - core[0]]


def order_weights(idx, core, ws):
    return pl.pallas_call(
        order_kernel,
        name="order_weights",
        grid=(1,),
        in_specs=[SMEM, SMEM] + [fixed(2, 384, 256)] * 8,
        out_specs=[fixed(8, 384, 256)] * 2,
        out_shape=[shape((8, 384, 256))] * 2,
        compiler_params=PARAMS,
    )(idx, core, *ws)


def upstream_kernel(idx, tok_idx, *refs):
    gs, ws, (out, ordered, wo) = refs[:8], refs[8:16], refs[16:]

    @pl.when(pl.program_id(0) == 0)
    def _():
        for n in range(8):
            for s in range(2):
                wo[tok_idx[n] * 2 + s] = ws[n][s]

    acc = jnp.zeros(out.shape, F32)
    for n in range(16):
        g = gs[n // 2][n % 2]
        ordered[idx[n]] = g
        acc = acc + dot(g, wo[idx[n]], NT)
    out[...] = acc.astype(BF16)


def upstream(idx, tok_idx, gs, ws):
    tile = 256
    return pl.pallas_call(
        upstream_kernel,
        name="upstream",
        grid=(512 // tile,),
        in_specs=[SMEM, SMEM]
        + [pl.BlockSpec((2, tile, 256), lambda i: (0, i, 0))] * 8
        + [pl.BlockSpec((2, 128, 256), lambda i: (0, 3, 0))] * 8,
        out_specs=[
            pl.BlockSpec((tile, 128), lambda i: (i, 0)),
            pl.BlockSpec((16, tile, 256), lambda i: (0, i, 0)),
            fixed(16, 128, 256),
        ],
        out_shape=[shape((512, 128)), shape((16, 512, 256)), shape((16, 128, 256))],
        compiler_params=PARAMS,
    )(idx, tok_idx, *gs, *ws)


KEY_BLOCK = 1024
SCALE = 1.0 / math.sqrt(128)
TO_BASE2 = SCALE * math.log2(math.e)


def masked_scores(b, kv, q, edge):
    s = dot(kv[pl.ds(b * KEY_BLOCK, KEY_BLOCK), 0:128], q[...], NT) * TO_BASE2
    pos = lax.broadcasted_iota(jnp.int32, s.shape, 0) + b * KEY_BLOCK
    return jnp.where(pos < edge, s, masked_low)


def forward_kernel(idx, limit, q, *refs):
    parts, (att, att_t, lse, kv, s_all) = refs[:8], refs[8:]
    for n in range(8):
        kv[pl.ds(idx[n] * 512, 512), :] = parts[n][...]
    count = kv.shape[0] // KEY_BLOCK
    cols = q.shape[0]
    edge = limit[...]

    def scores(b, top):
        s = masked_scores(b, kv, q, edge)
        s_all[pl.ds(b * KEY_BLOCK, KEY_BLOCK), :] = s
        return jnp.maximum(top, jnp.max(s, axis=0, keepdims=True))

    top = lax.fori_loop(0, count, scores, jnp.full((1, cols), masked_low, F32), unroll=4)

    def sums(b, total):
        at = pl.ds(b * KEY_BLOCK, KEY_BLOCK)
        e = jnp.exp2(s_all[at, :] - top)
        s_all[at, :] = e
        return total + jnp.sum(e, axis=0, keepdims=True)

    total = lax.fori_loop(0, count, sums, jnp.zeros((1, cols), F32), unroll=4)
    inv = 1.0 / total
    lse[...] = top + jnp.log2(total)

    def attend(b, acc):
        at = pl.ds(b * KEY_BLOCK, KEY_BLOCK)
        return acc + dot(kv[at, 128:256], (s_all[at, :] * inv).astype(BF16), TN)

    out_t = lax.fori_loop(0, count, attend, jnp.zeros((128, cols), F32), unroll=4).astype(BF16)
    att_t[...] = out_t
    att[...] = out_t.T


def forward(idx, limit, q, parts):
    vmem = pl.BlockSpec(memory_space=pltpu.VMEM)
    return pl.pallas_call(
        forward_kernel,
        name="forward",
        in_specs=[SMEM] + [vmem] * 10,
        out_shape=[shape((512, 128)), shape((128, 512)), shape((1, 512), F32), shape((4096, 256))],
        scratch_shapes=[pltpu.VMEM((4096, 512), F32)],
        compiler_params=PARAMS,
    )(idx, limit, q, *parts)


def backward_kernel(limit, lse, q, kv, da, att_t, dq, dkv):
    count = kv.shape[0] // KEY_BLOCK
    edge = limit[...]
    da_t = da[...].T
    row_dots = jnp.sum(att_t[...].astype(F32) * da_t.astype(F32), axis=0, keepdims=True)

    def back(b, acc):
        at = pl.ds(b * KEY_BLOCK, KEY_BLOCK)
        p = jnp.exp2(masked_scores(b, kv, q, edge) - lse[...])
        d_probs = dot(kv[at, 128:256], da[...], NT)
        ds = (p * (d_probs - row_dots) * SCALE).astype(BF16)
        dkv[at, 0:128] = dot(ds, q[...]).astype(BF16)
        dkv[at, 128:256] = dot(p.astype(BF16), da[...]).astype(BF16)
        return acc + dot(kv[at, 0:128], ds, TN)

    dq_t = lax.fori_loop(0, count, back, jnp.zeros((128, q.shape[0]), F32), unroll=2)
    dq[...] = dq_t.astype(BF16).T


def backward(limit, lse, q, kv, da, att_t):
    return pl.pallas_call(
        backward_kernel,
        name="backward",
        out_shape=[shape((512, 128)), shape((4096, 256))],
        compiler_params=PARAMS,
    )(limit, lse, q, kv, da, att_t)


def split_rows(dots):
    rows = []
    for p in (dots[:, 0:256], dots[:, 256:512]):
        high = p.astype(BF16).astype(F32)
        mid = (p - high).astype(BF16).astype(F32)
        rows.append((high, mid, p - high - mid))
    kind = lax.broadcasted_iota(jnp.int32, (16, 256), 0)
    both = jnp.zeros((16, 256), F32)
    for r in range(6):
        both = jnp.where(kind == r, rows[r % 2][r // 2], both)
    return both.astype(BF16)


def joined_rows(block):
    t = block.astype(F32)
    return (t[0:2] + t[2:4]) + t[4:6]


def gradients_kernel(idx, dkv, dq, q, kv, n0, n1, w0, w1, g_out, dots, up, down, far, far_next, here, g_t):
    step = pl.program_id(0)

    @pl.when(step == 0)
    def _():
        total = dkv[0].astype(F32)
        for k in range(1, 8):
            total = total + dkv[k].astype(F32)
        g = jnp.concatenate([dq[...], total.astype(BF16)], axis=1)
        g_out[...] = g
        g_t[...] = g.T
        gf = g.astype(F32)
        prod = gf[:, 0:128] * q[...].astype(F32)
        prod = prod + gf[:, 128:256] * kv[:, 0:128].astype(F32)
        prod = prod + gf[:, 256:384] * kv[:, 128:256].astype(F32)
        ones = jnp.ones((8, 128), F32)
        dots[...] = lax.dot_general(
            ones, prod, NT, precision=lax.Precision.HIGHEST, preferred_element_type=F32
        )

    outs = ((up.at[0], up.at[1]), (down.at[0], down.at[1]), (far, far_next), (here.at[0], here.at[1]))
    for n, pair in enumerate(outs):

        @pl.when(step == n + 1)
        def _(pair=pair):
            for out, block, wo in ((pair[0], n0, w0), (pair[1], n1, w1)):
                for k in range(2):
                    out[k, 0:384, :] = dot(g_t[...], block[k]).astype(BF16)
                    out[k, 384:512, :] = wo[k]


def gradients(idx, dkv, dq, q, kv, normed, dwo):
    at = lambda slot: lambda i, idx: (idx[2 * jnp.maximum(i - 1, 0) + slot], 0, 0)
    spec = pltpu.PrefetchScalarGridSpec(
        num_scalar_prefetch=1,
        grid=(5,),
        in_specs=[
            fixed(8, 512, 256),
            fixed(512, 128),
            fixed(512, 128),
            fixed(512, 256),
            pl.BlockSpec((2, 512, 256), at(0)),
            pl.BlockSpec((2, 512, 256), at(1)),
            pl.BlockSpec((2, 128, 256), at(0)),
            pl.BlockSpec((2, 128, 256), at(1)),
        ],
        out_specs=[
            fixed(512, 384),
            fixed(8, 512),
            fixed(2, 2, 512, 256),
            fixed(2, 2, 512, 256),
            fixed(2, 512, 256),
            fixed(2, 512, 256),
            fixed(2, 2, 512, 256),
        ],
        scratch_shapes=[pltpu.VMEM((384, 512), BF16)],
    )
    return pl.pallas_call(
        gradients_kernel,
        name="gradients",
        grid_spec=spec,
        out_shape=[
            shape((512, 384)),
            shape((8, 512), F32),
            shape((2, 2, 512, 256)),
            shape((2, 2, 512, 256)),
            shape((2, 512, 256)),
            shape((2, 512, 256)),
            shape((2, 2, 512, 256)),
        ],
        compiler_params=PARAMS,
    )(idx, dkv, dq, q, kv, normed, normed, dwo, dwo)


def add_kernel(*refs):
    total = refs[0][...].astype(F32)
    for t in refs[1:-1]:
        total = total + t[...].astype(F32)
    refs[-1][...] = total.astype(BF16)


def add_blocks(terms, specs):
    return pl.pallas_call(
        add_kernel,
        name="add_blocks",
        grid=(2,),
        in_specs=specs,
        out_specs=pl.BlockSpec((None, 512, 256), lambda i: (i, 0, 0)),
        out_shape=shape((2, 512, 256)),
        compiler_params=PARAMS,
    )(*terms)


def input_grad_kernel(idx, g, g2, w, w2, dots, dots2, *outs):
    rows = split_rows(dots[0:1] + dots2[0:1])
    for n in range(8):
        out, at = outs[n // 2], idx[n]
        both = dot(g[...], w[at]) + dot(g2[...], w2[at])
        out[n % 2, 0:512, :] = both.astype(BF16)
        out[n % 2, 512:528, :] = rows


def input_grad(idx, g, g2, w, w2, dots, dots2):
    vmem = pl.BlockSpec(memory_space=pltpu.VMEM)
    return pl.pallas_call(
        input_grad_kernel,
        name="input_grad",
        in_specs=[SMEM] + [vmem] * 6,
        out_shape=[shape((2, 528, 256))] * 4,
        compiler_params=PARAMS,
    )(idx, g, g2, w, w2, dots, dots2)


def weight_grad_kernel(left, right, out):
    for k in range(right.shape[0]):
        out[k] = dot(left[...], right[k]).astype(BF16)


def weight_grad(left, right):
    rows = left.shape[0]
    return pl.pallas_call(
        weight_grad_kernel,
        name="weight_grad",
        grid=(2,),
        in_specs=[fixed(rows, 512), pl.BlockSpec((8, 512, 256), lambda j: (j, 0, 0))],
        out_specs=pl.BlockSpec((8, rows, 256), lambda j: (j, 0, 0)),
        out_shape=shape((16, rows, 256)),
        compiler_params=PARAMS,
    )(left, right)


def line_kernel(side, *refs):
    terms, (x, x_next, inv, mod, own, own_dots, sent, gains) = refs[:4], refs[4:]
    second = mod[...] == 1
    for slot, block in ((0, x), (1, x_next)):
        total = terms[0][slot, 0:512].astype(F32)
        dots = joined_rows(terms[0][slot, 512:528])
        for t in terms[1:]:
            total = total + t[slot, 0:512].astype(F32)
            dots = dots + joined_rows(t[slot, 512:528])
        if slot == 0:
            own[...] = total
            own_dots[0:2] = dots
        else:
            sent[0:512] = total.astype(BF16)
            sent[512:528] = split_rows(jnp.concatenate([dots[0:1], dots[1:2]], axis=1))
        each = total * (block[...].astype(F32) * inv[...])
        first = jnp.sum(jnp.where(second, 0.0, each), axis=0, keepdims=True)
        other = jnp.sum(jnp.where(second, each, 0.0), axis=0, keepdims=True)
        at = side[0] if slot == 0 else 1 - side[0]
        for k in range(8):
            gains[k, at, 0:1] = first
            gains[k, at, 1:2] = other


NEXT = pl.BlockSpec((None, 512, 256), lambda i: (1, 0, 0))


def line_sum(side, terms, x, x_next, inv, modality):
    return pl.pallas_call(
        line_kernel,
        name="line_sum",
        grid=(1,),
        in_specs=[SMEM]
        + [fixed(2, 528, 256)] * 4
        + [fixed(512, 256), NEXT, fixed(512, 1), fixed(512, 1)],
        out_specs=[fixed(512, 256), fixed(8, 256), fixed(528, 256), fixed(8, 2, 2, 256)],
        out_shape=[
            shape((512, 256), F32),
            shape((8, 256), F32),
            shape((528, 256)),
            shape((8, 2, 2, 256), F32),
        ],
        compiler_params=PARAMS,
    )(side, *terms, x, x_next, inv, modality)


def finish_kernel(own, own_dots, last, x, inv, mod, gain, grad_in):
    gn = own[...] + last[0:512].astype(F32)
    dots = own_dots[0:2] + joined_rows(last[512:528])
    columns = [jnp.broadcast_to(dots[r : r + 1], (128, 256)).T[:, 0:1] for r in range(2)]
    mean = jnp.concatenate(columns, axis=0) / 4096
    scaled = x[...].astype(F32) * inv[...]
    up = gn * jnp.where(mod[...] == 1, gain[1:2], gain[0:1])
    grad_in[...] = (inv[...] * (up - scaled * mean)).astype(BF16)


def finish(own, own_dots, last, x, inv, modality, gain):
    return pl.pallas_call(
        finish_kernel,
        name="finish",
        out_shape=shape((512, 256)),
        compiler_params=PARAMS,
    )(own, own_dots, last, x, inv, modality, gain)


def output_kernel(idx, *refs):
    atts, (rows, out) = refs[:8], refs[8:]
    total = jnp.zeros(out.shape, F32)
    for n in range(16):
        total = total + dot(atts[n // 2][n % 2], rows[idx[n]]).astype(BF16).astype(F32)
    out[...] = total.astype(BF16)


def output(idx, atts, rows):
    tile = 128
    return pl.pallas_call(
        output_kernel,
        name="output",
        grid=(512 // tile,),
        in_specs=[SMEM]
        + [pl.BlockSpec((2, tile, 128), lambda i: (0, i, 0))] * 8
        + [fixed(16, 128, 256)],
        out_specs=pl.BlockSpec((tile, 256), lambda i: (i, 0)),
        out_shape=shape((512, 256)),
        compiler_params=PARAMS,
    )(idx, *atts, rows)


def sum_weights_kernel(*refs):
    parts, (qkv, wout) = refs[:5], refs[5:]
    total = parts[0][...].astype(F32)
    for t in parts[1:]:
        total = total + t[...].astype(F32)
    for m in range(3):
        qkv[m] = total[m * 128 : (m + 1) * 128].T
    wout[...] = total[384:512]


ONE = pl.BlockSpec((None, 512, 256), lambda i: (i, 0, 0))
FIRST = pl.BlockSpec((None, None, 512, 256), lambda i: (0, i, 0, 0))
SECOND = pl.BlockSpec((None, None, 512, 256), lambda i: (1, i, 0, 0))


def sum_weights(parts):
    return pl.pallas_call(
        sum_weights_kernel,
        name="sum_weights",
        grid=(2,),
        in_specs=[FIRST, FIRST, FIRST, ONE, ONE],
        out_specs=[
            pl.BlockSpec((3, 256, 128), lambda s: (0, s, 0)),
            pl.BlockSpec((128, 256), lambda s: (0, s)),
        ],
        out_shape=[shape((3, 512, 128), F32), shape((128, 512), F32)],
        compiler_params=PARAMS,
    )(*parts)


def sublayer(layer_input, modality, image_spans, norm_gain, w_qkv, w_out, grad_out):
    x, h, c = (lax.axis_index(a) for a in GROUP)
    z, u = (lax.axis_index(a) for a in TOKENS_AXES)
    blocks = [((x - d) % 4, h ^ s, c ^ k) for k in range(2) for d in TURNS for s in range(2)]
    idx = jnp.stack([a * 4 + b * 2 + e for a, b, e in blocks]).astype(jnp.int32)
    tok_idx = jnp.stack([((z - d) % 4) * 2 + (u ^ s) for s in range(2) for d in TURNS]).astype(jnp.int32)
    places = jnp.stack([((x + d) % 4) * 2 + (h ^ s) for d in range(4) for s in range(2)]).astype(jnp.int32)
    outward = [((z + d) % 4) * 2 + (u ^ s) for d in (1, 3, 2, 0) for s in range(2)]
    out_idx = jnp.stack(outward).astype(jnp.int32)
    core = c.astype(jnp.int32)[None]
    side = h.astype(jnp.int32)[None]
    column = modality[:, None]

    gain_rows = jnp.concatenate(three_parts(norm_gain), axis=0).astype(BF16)
    gain_rows = jnp.concatenate([gain_rows, jnp.zeros((10, 256), BF16)], axis=0)
    xs = spread(jnp.concatenate([layer_input, gain_rows], axis=0))
    ws = gather_tokens_axes(pack_weights(w_qkv, w_out))
    gs = spread(grad_out)

    normed, inv = normalize(idx, xs, column)
    q, kv = project(tok_idx, normed, ws)
    kvs = gather_tokens_axes(kv)
    w_kept, w_sent = order_weights(tok_idx, core, ws)
    w_other = swap(w_sent, "c")
    da, g_all, wo = upstream(idx, tok_idx, gs, ws)

    pos = (z * 2 + u) * 512 + jnp.arange(512, dtype=jnp.int32)
    inside = (pos[:, None] >= image_spans[0][None]) & (pos[:, None] < image_spans[1][None])
    ends = jnp.max(jnp.where(inside, image_spans[1][None], 0), axis=1)
    limit = jnp.maximum(pos + 1, ends)[None, :]

    out_rows = exchange(wo, GROUP)
    att, att_t, lse, all_kv = forward(tok_idx, limit, q, kvs)
    dq, dkv = backward(limit, lse, q, all_kv, da, att_t)
    dkv_parts = exchange(dkv.reshape(8, 512, 256), TOKENS_AXES)

    dwo = weight_grad(att_t, g_all)
    atts = spread(att)
    attn_out = output(idx, atts, out_rows)

    g, dots, up, down, far, far_next, here = gradients(out_idx, dkv_parts, dq, q, kv, normed, dwo)
    far_next = swap(far_next, "u")
    up, down = turn(up, 1, "z"), turn(down, 3, "z")
    far = turn(add_blocks([far, far_next], [ONE, ONE]), 2, "z")
    across = swap(add_blocks([here, up, down], [SECOND] * 3), "u")
    g2, dots2 = swap(g, "c"), swap(dots, "c")
    terms = input_grad(places, g, g2, w_kept, w_other, dots, dots2)
    terms = [turn(t, d) if d else t for d, t in enumerate(terms)]
    own, own_dots, sent, gains = line_sum(side, terms, layer_input, xs[0], inv, column)
    last = swap(sent, "h")
    gains = exchange(gains.reshape(16, 2, 256), ("z", "u", "h"))
    grad_in = finish(own, own_dots, last, layer_input, inv, column, norm_gain)
    grad_qkv, grad_wout = sum_weights([here, up, down, far, across])
    grad_gain = jnp.sum(gains, axis=0)
    return (attn_out, grad_in, grad_qkv, grad_wout, grad_gain)


def solution(mesh):
    fine = Mesh(mesh.devices.reshape(4, 2, 2, 4, 2), ("x", "h", "c", "z", "u"))
    tok, feat = TOKENS_AXES, GROUP
    in_specs = (P(tok, feat), P(tok), P(), P(None, feat), P(None, tok, feat), P(feat, tok), P(tok, feat))
    out_specs = (P(tok, feat), P(tok, feat), P(None, tok, feat), P(feat, tok), P(None, feat))
    return jax.shard_map(sublayer, mesh=fine, in_specs=in_specs, out_specs=out_specs, check_vma=False)
```
